32 devices in a mesh: gx: 4 (over x, core), gy: 8 (over z, y).
Axes of the slice: x: 2, y: 2, z: 4, core: 2. Of those that a mesh axis runs over, the one named last changes fastest.
Arguments:
- electric: float32 [3, 64, 128, 256], P(None, 'gx', 'gy'), may hold values from -6 to 6
- magnetic: float32 [3, 64, 128, 256], P(None, 'gx', 'gy'), may hold values from -6 to 6
- aux_electric: float32 [6, 64, 128, 256], P(None, 'gx', 'gy'), may hold values from -3 to 3
- aux_magnetic: float32 [6, 64, 128, 256], P(None, 'gx', 'gy'), may hold values from -3 to 3
- grades: int32 [3, 64, 128, 256], P(None, 'gx', 'gy'), may hold values from 0 to 3
- permittivity: float32 [64, 128, 256], P('gx', 'gy'), may hold values from 1 to 8
- dipole_cell: int32 [3, 16384], P(None, ('gx', 'gy')), may hold values from 0 to 255, as said below
- dipole_port: int32 [16384], P(('gx', 'gy')), may hold values from 0 to 511
- live_count: int32 [32], P(('gx', 'gy')), may hold values from 1 to 512, as said below
- injection: bfloat16 [16384, 512], P(('gx', 'gy')), may hold values from -0.25 to 0.25
- waveform: bfloat16 [512, 16], replicated, may hold values from -6 to 6
Outputs:
- electric_out: float32 [3, 64, 128, 256], P(None, 'gx', 'gy')
- magnetic_out: float32 [3, 64, 128, 256], P(None, 'gx', 'gy')
- port_power: float32 [16, 512], replicated
The draws below stay inside these ranges and needn't reach their ends.
Inputs may be any that keep to these rules, and one draw needn't show every extreme that they name: `dipole_cell`: slot s lies in the block of cells held by the device that holds slot s. The live slots of a device are its first live_count ones; some device has all 512 live.
All inputs are finite; a program needn't handle non-finite values.
Results may differ from the reference program's by a relative error of at most 0.0003.
Values sent between devices are 32-bit elements; how exact they have to be, the bound alone decides.
A program may use at most 128 MiB of HBM per device.

```python
import math
import jax
import jax.numpy as jnp
from jax import lax

CX = 16
CY = 16
NZ = 256
DIP_DEV = 512
STEPS = 16
PORTS = 512
NX = 64
NY = 128
DIPOLES = 16384


def draw_dipole_cell(key, part):
    across = NY // CY
    slots = jnp.arange(DIPOLES, dtype=jnp.int32)
    owner = slots // DIP_DEV
    row_block = owner // across
    col_block = owner % across
    key_x, key_y, key_z = jax.random.split(jax.random.fold_in(key, 11), 3)
    coord_x = row_block * CX + jax.random.randint(key_x, (DIPOLES,), 0, CX)
    coord_y = col_block * CY + jax.random.randint(key_y, (DIPOLES,), 0, CY)
    coord_z = jax.random.randint(key_z, (DIPOLES,), 0, NZ)
    return jnp.stack([coord_x, coord_y, coord_z]).astype(jnp.int32)


def draw_dipole_port(key, part):
    devices = DIPOLES // DIP_DEV
    share = PORTS // devices
    slots = jnp.arange(DIPOLES, dtype=jnp.int32)
    owner = slots // DIP_DEV
    key_near, key_far, key_pick = jax.random.split(jax.random.fold_in(key, 23), 3)
    near = owner * share + jax.random.randint(key_near, (DIPOLES,), 0, share)
    far = jax.random.randint(key_far, (DIPOLES,), 0, PORTS)
    pick = jax.random.randint(key_pick, (DIPOLES,), 0, 4)
    return jnp.where(pick == 0, far, near).astype(jnp.int32)


def draw_live_count(key, part):
    devices = DIPOLES // DIP_DEV
    key_one, key_two, key_full = jax.random.split(jax.random.fold_in(key, 37), 3)
    first = jax.random.randint(key_one, (devices,), 1, DIP_DEV + 1)
    second = jax.random.randint(key_two, (devices,), 1, DIP_DEV + 1)
    counts = jnp.minimum(first, second)
    full = jax.random.randint(key_full, (), 0, devices)
    return jnp.where(jnp.arange(devices) == full, DIP_DEV, counts).astype(jnp.int32)


def place_ends(values, own_key, least, top_value):
    spot = [jax.random.randint(jax.random.fold_in(own_key, axis), (), 0, length) for axis, length in enumerate(values.shape)]
    main_axis = values.shape.index(max(values.shape))
    next_to = spot[:main_axis] + [(spot[main_axis] + 1) % values.shape[main_axis]] + spot[main_axis + 1:]
    return values.at[tuple(spot)].set(least).at[tuple(next_to)].set(top_value)


def block_levels(rng, extent, cuts, least, top_value):
    loudness = 1.0
    for dim, blocks in cuts:
        steps = jax.random.uniform(jax.random.fold_in(jax.random.fold_in(rng, 6), dim), (blocks,), jnp.float32, least / len(cuts), top_value / len(cuts))
        loudness = loudness * jnp.repeat(jnp.exp(steps), extent[dim] // blocks).reshape((-1,) + (1,) * (len(extent) - 1 - dim))
    return loudness


def normal_values(rng, shape, width, limit, cuts=(), kind=jnp.bfloat16):
    values = jax.random.normal(rng, shape, jnp.float32) * width
    if len(cuts) > 0:
        values = block_levels(rng, shape, cuts, -0.22, 0.18) * values
    return jnp.clip(values, min=-limit, max=limit).astype(kind)


def setup_inputs(seed: int = 0) -> dict:
    keys = jax.random.split(jax.random.key(seed), 12)
    electric = normal_values(keys[0], (3, NX, NY, NZ), 1.0, 6.0, ((1, 4), (2, 8)), jnp.float32)
    magnetic = normal_values(keys[1], (3, NX, NY, NZ), 1.0, 6.0, ((1, 4), (2, 8)), jnp.float32)
    aux_electric = normal_values(keys[2], (6, NX, NY, NZ), 0.4, 3.0, ((1, 4), (2, 8)), jnp.float32)
    aux_magnetic = normal_values(keys[3], (6, NX, NY, NZ), 0.4, 3.0, ((1, 4), (2, 8)), jnp.float32)
    grades = place_ends(jax.random.randint(keys[4], (3, NX, NY, NZ), 0, 4), jax.random.fold_in(keys[4], 1), 0, 3).astype(jnp.int32)
    permittivity = jnp.clip(jnp.exp(math.log(8.0) - 2.0794415 * jax.random.uniform(keys[5], (NX, NY, NZ), jnp.float32) ** block_levels(keys[5], (NX, NY, NZ), ((0, 4), (1, 8)), -0.2, 0.2)), 1.0, 8.0)
    dipole_cell = draw_dipole_cell(jax.random.fold_in(keys[11], 71), 0)
    dipole_port = draw_dipole_port(jax.random.fold_in(keys[11], 71), 0)
    live_count = draw_live_count(jax.random.fold_in(keys[11], 71), 0)
    injection = normal_values(keys[9], (DIPOLES, PORTS), PORTS ** -0.5, 0.25, ((0, 32),))
    waveform = normal_values(keys[10], (PORTS, STEPS), 1.0, 6.0)
    return dict(electric=electric, magnetic=magnetic, aux_electric=aux_electric, aux_magnetic=aux_magnetic, grades=grades, permittivity=permittivity, dipole_cell=dipole_cell, dipole_port=dipole_port, live_count=live_count, injection=injection, waveform=waveform)


courant = 0.55
absorb_keep = (0.0, 0.92, 0.75, 0.45)
absorb_take = (0.0, -0.06, -0.18, -0.35)
derivative_pairs = ((2, 1), (1, 2), (0, 2), (2, 0), (1, 0), (0, 1))


def difference(values, axis, plane, forward):
    length = values.shape[axis]
    if plane is None:
        shape = list(values.shape)
        shape[axis] = 1
        plane = jnp.zeros(shape, values.dtype)
    if forward:
        after = jnp.concatenate([lax.slice_in_dim(values, 1, length, axis=axis), plane], axis)
        return after - values
    before = jnp.concatenate([plane, lax.slice_in_dim(values, 0, length - 1, axis=axis)], axis)
    return values - before


def grade_table(grades, table):
    result = jnp.zeros(grades.shape, jnp.float32)
    for level in range(1, 4):
        result = result + jnp.where(grades == level, table[level], 0.0)
    return result


def curl(field, auxiliary, keep, take, planes, forward):
    terms = []
    updated = []
    for number, (component, axis) in enumerate(derivative_pairs):
        plane = None
        if planes is not None and axis == 0:
            plane = planes[0][component - 1]
        if planes is not None and axis == 1:
            plane = planes[1][component // 2]
        slope = difference(field[component], axis, plane, forward)
        carried = keep[axis] * auxiliary[number] + take[axis] * slope
        terms.append(slope + carried)
        updated.append(carried)
    rotation = jnp.stack([terms[0] - terms[1], terms[2] - terms[3], terms[4] - terms[5]])
    return rotation, jnp.stack(updated)


def reference(electric, magnetic, aux_electric, aux_magnetic, grades, permittivity, dipole_cell, dipole_port, live_count, injection, waveform):
    keep = grade_table(grades, absorb_keep)
    take = grade_table(grades, absorb_take)
    slots = jnp.arange(DIPOLES, dtype=jnp.int32)
    live = ((slots % DIP_DEV) < live_count[slots // DIP_DEV]).astype(jnp.float32)
    current = jnp.dot(injection, waveform, preferred_element_type=jnp.float32) * live[:, None]
    flat_cell = (dipole_cell[0] * (NY * NZ) + dipole_cell[1] * NZ + dipole_cell[2]).astype(jnp.int32)
    factor = courant / permittivity
    powers = []
    for step in range(STEPS):
        rotation, aux_electric = curl(electric, aux_electric, keep, take, None, True)
        magnetic = magnetic - courant * rotation
        rotation, aux_magnetic = curl(magnetic, aux_magnetic, keep, take, None, False)
        electric = electric + factor * rotation
        current_now = current[:, step]
        flat_z = electric[2].reshape(-1).at[flat_cell].add(-courant * current_now)
        drive = current_now * flat_z[flat_cell]
        electric = jnp.concatenate([electric[0:2], flat_z.reshape(1, NX, NY, NZ)], 0)
        powers.append(jax.ops.segment_sum(drive, dipole_port, PORTS))
    return electric, magnetic, jnp.stack(powers)
```

```python
import functools

import jax
import jax.numpy as jnp
from jax import lax
from jax.experimental import pallas as pl
from jax.experimental.pallas import tpu as pltpu
from jax.sharding import PartitionSpec as P

MESH = pl.DeviceIdType.MESH
courant = 0.55
absorb_keep = (0.0, 0.92, 0.75, 0.45)
absorb_take = (0.0, -0.06, -0.18, -0.35)
derivative_pairs = ((2, 1), (1, 2), (0, 2), (2, 0), (1, 0), (0, 1))
UNROLL = 4


def grade_table(grades, table):
    result = jnp.where(grades == 1, table[1], 0.0)
    result = jnp.where(grades == 2, table[2], result)
    return jnp.where(grades == 3, table[3], result)


def split_two(values):
    high = values.astype(jnp.bfloat16)
    low = (values - high.astype(jnp.float32)).astype(jnp.bfloat16)
    return high, low


KINDS = ("ay", "by", "axh", "axl", "bxl", "bxh", "d1", "d2")
TRAVEL = {
    "ay": (0, 1), "by": (0, -1), "axh": (1, 0), "axl": (1, 0),
    "bxl": (-1, 0), "bxh": (-1, 0), "d1": (-1, 1), "d2": (1, -1),
}
COEFFICIENTS = ((0, 1), (0, -1), (1, 0), (-1, 0), (-1, 1), (1, -1))
SLOTS = 4


def kernel(
    e_in, h_in, me_in, mh_in, grades_ref, eps_ref, cell_ref, port_ref, live_ref, inj_ref, wave_ref,
    e_out, h_out, power_ref,
    ef, hf, me, mh, keep, take, factor, source,
    say, sby, saxh, saxl, sbxl, sbxh, sd1, sd2,
    ray, rby, raxh, raxl, rbxl, rbxh, rd1, rd2,
    cs_up, cs_down, cs_right, cs_left, cs_d1, cs_d2,
    cr_up, cr_down, cr_right, cr_left, cr_d1, cr_d2,
    row_h, row_e, save_row_h, save_row_e, save_h_lo, save_h_hi, save_e_lo, save_e_hi, lines,
    edge_h, edge_ht, edge_e, edge_et,
    cell_t, cell_f, depth_t, depth, current, record, z_copy,
    share, from_y, from_x, result,
    load_sem, store_sem, send_sem, recv_sem, send_one, recv_one, send_sum, recv_sum,
):
    depth_x, depth_y, depth_z = eps_ref.shape
    ports, slots = inj_ref.shape[1], inj_ref.shape[0]
    steps = wave_ref.shape[0]
    half = depth_y // 2
    last_x, last_y = depth_x - 1, depth_y - 1
    ix, iy = lax.axis_index("gx"), lax.axis_index("gy")
    count_x, count_y = lax.axis_size("gx"), lax.axis_size("gy")
    f32 = jnp.float32

    def there(dx, dy):
        found = ix >= 0
        if dx:
            found = jnp.logical_and(found, ix > 0 if dx < 0 else ix < count_x - 1)
        if dy:
            found = jnp.logical_and(found, iy > 0 if dy < 0 else iy < count_y - 1)
        return found

    loads = [
        pltpu.make_async_copy(e_in, ef.at[:, pl.ds(0, depth_x)], load_sem.at[0]),
        pltpu.make_async_copy(h_in, hf.at[:, pl.ds(1, depth_x)], load_sem.at[1]),
        pltpu.make_async_copy(me_in, me, load_sem.at[2]),
        pltpu.make_async_copy(mh_in, mh, load_sem.at[3]),
    ]
    for copy in loads:
        copy.start()

    plane = jnp.zeros((depth_y, depth_z), f32)
    for component in range(3):
        ef[component, depth_x] = plane
        hf[component, 0] = plane
    for ref in (
        ray, rby, raxh, raxl, rbxl, rbxh, rd1, rd2,
        cr_up, cr_down, cr_right, cr_left, cr_d1, cr_d2,
        save_row_h, save_h_lo, save_h_hi, lines, sd2, cs_up, cs_down, cs_right, cs_left, cs_d1, cs_d2,
    ):
        ref[...] = jnp.zeros(ref.shape, f32)

    barrier = pltpu.get_barrier_semaphore()
    line_x = [(lax.rem(ix + offset, count_x), iy) for offset in range(1, count_x)]
    line_y = [(ix, lax.rem(iy + offset, count_y)) for offset in range(1, count_y)]
    across = [
        (lax.rem(ix + count_x - 1, count_x), lax.rem(iy + 1, count_y)),
        (lax.rem(ix + 1, count_x), lax.rem(iy + count_y - 1, count_y)),
    ]
    for peer in line_x + line_y + across:
        pl.semaphore_signal(barrier, inc=1, device_id=peer, device_id_type=MESH)

    def prepare(x, _):
        for d in range(3):
            level = grades_ref[d, x]
            keep[d, x] = grade_table(level, absorb_keep)
            take[d, x] = grade_table(level, absorb_take)
        factor[x] = courant / eps_ref[x]
        return 0

    lax.fori_loop(0, depth_x, prepare, 0)

    row_half = lax.broadcasted_iota(jnp.int32, (half, depth_z), 0)
    is_top, is_bottom = row_half == half - 1, row_half == 0

    for x in range(depth_x):
        upper = take[1, x, half:, :]
        lower = take[1, x, :half, :]
        scale_h = courant * (1.0 + upper)
        scale_e = factor[x, :half, :] * (1.0 + lower)
        edge_h[x] = jnp.where(is_top, scale_h, 0.0)
        edge_ht[x] = jnp.where(is_top, upper, 0.0)
        edge_e[x] = jnp.where(is_bottom, scale_e, 0.0)
        edge_et[x] = jnp.where(is_bottom, lower, 0.0)
        cs_up[x:x + 1, :] = scale_h[half - 1:half, :]
        cs_down[x:x + 1, :] = scale_e[0:1, :]
    cs_right[0:depth_y, :] = courant * (1.0 + take[0, last_x])
    cs_left[0:depth_y, :] = factor[0] * (1.0 + take[0, 0])
    cs_up[depth_x:depth_x + 1, :] = cs_right[last_y:depth_y, :]
    cs_down[depth_x:depth_x + 1, :] = cs_left[0:1, :]
    cs_right[depth_y:depth_y + 1, :] = cs_up[last_x:depth_x, :]
    cs_left[depth_y:depth_y + 1, :] = cs_down[0:1, :]
    cs_d1[0:1, :] = cs_up[0:1, :]
    cs_d2[0:1, :] = cs_down[last_x:depth_x, :]

    once = []
    for number, (source_ref, target_ref) in enumerate((
        (cs_up, cr_up), (cs_down, cr_down), (cs_right, cr_right),
        (cs_left, cr_left), (cs_d1, cr_d1), (cs_d2, cr_d2),
    )):
        dx, dy = COEFFICIENTS[number]
        once.append((there(dx, dy), there(-dx, -dy), pltpu.make_async_remote_copy(
            src_ref=source_ref, dst_ref=target_ref,
            send_sem=send_one.at[number], recv_sem=recv_one.at[number],
            device_id=(ix + dx, iy + dy), device_id_type=MESH)))

    sends = dict(ay=say, by=sby, axh=saxh, axl=saxl, bxl=sbxl, bxh=sbxh, d1=sd1, d2=sd2)
    gets = dict(ay=ray, by=rby, axh=raxh, axl=raxl, bxl=rbxl, bxh=rbxh, d1=rd1, d2=rd2)

    def message(kind, step):
        number = KINDS.index(kind)
        slot = lax.rem(step, SLOTS)
        dx, dy = TRAVEL[kind]
        return pltpu.make_async_remote_copy(
            src_ref=sends[kind], dst_ref=gets[kind].at[slot],
            send_sem=send_sem.at[number], recv_sem=recv_sem.at[number, slot],
            device_id=(ix + dx, iy + dy), device_id_type=MESH)

    def send(step, *kinds):
        for kind in kinds:
            dx, dy = TRAVEL[kind]
            pl.when(there(dx, dy))(message(kind, step).start)

    def sent(step, *kinds):
        for kind in kinds:
            dx, dy = TRAVEL[kind]
            pl.when(there(dx, dy))(message(kind, step).wait_send)

    def arrived(step, *kinds):
        for kind in kinds:
            dx, dy = TRAVEL[kind]
            pl.when(there(-dx, -dy))(message(kind, step).wait_recv)

    low, high = slice(0, half), slice(half, depth_y)
    lanes = lax.broadcasted_iota(jnp.int32, (half, depth_z), 1)
    z_last, z_first = lanes == depth_z - 1, lanes == 0

    def curl(x, part, here, beside, line, memory, forward):
        turn_y = half - 1 if forward else 1
        turn_z = depth_z - 1 if forward else 1
        edge_y = is_top if forward else is_bottom
        edge_z = z_last if forward else z_first
        terms = []
        for number, (component, axis) in enumerate(derivative_pairs):
            value = here[component]
            if axis == 0:
                other = beside[component]
            elif axis == 1:
                other = jnp.where(edge_y, line[component], pltpu.roll(value, turn_y, 0))
            else:
                other = jnp.where(edge_z, 0.0, pltpu.roll(value, turn_z, 1))
            slope = other - value if forward else value - other
            carried = keep[axis, x, part] * memory[number, x, part] + take[axis, x, part] * slope
            memory[number, x, part] = carried
            terms.append(slope + carried)
        return (terms[0] - terms[1], terms[2] - terms[3], terms[4] - terms[5])

    blocks = depth_x // UNROLL
    no_line = [0.0, None, 0.0]

    def update_h(upper):
        part = high if upper else low

        def run(block, _):
            for inner in range(UNROLL):
                x = block * UNROLL + inner
                here = [ef[c, x, part] for c in range(3)]
                beside = [None, ef[1, x + 1, part], ef[2, x + 1, part]]
                line = no_line
                if not upper:
                    line = [ef[0, x, half:half + 1, :], None, ef[2, x, half:half + 1, :]]
                rotation = curl(x, part, here, beside, line, me, True)
                fresh = [hf[c, x + 1, part] - courant * rotation[c] for c in range(3)]
                for c in range(3):
                    hf[c, x + 1, part] = fresh[c]
                z_copy[x, part] = here[2]
                if upper:
                    say[0, pl.ds(x, 1), :] = fresh[0][half - 1:half, :]
                    say[1, pl.ds(x, 1), :] = fresh[2][half - 1:half, :]
            return 0

        lax.fori_loop(0, blocks, run, 0)

    def update_e(upper):
        part = high if upper else low

        def run(block, _):
            for inner in range(UNROLL):
                x = block * UNROLL + inner
                here = [hf[c, x + 1, part] for c in range(3)]
                beside = [None, hf[1, x, part], hf[2, x, part]]
                line = no_line
                if upper:
                    line = [hf[0, x + 1, half - 1:half, :], None, hf[2, x + 1, half - 1:half, :]]
                rotation = curl(x, part, here, beside, line, mh, False)
                ratio = factor[x, part]
                fresh = [ef[c, x, part] + ratio * rotation[c] for c in range(3)]
                fresh[2] = fresh[2] - source[x, part]
                for c in range(3):
                    ef[c, x, part] = fresh[c]
                if not upper:
                    sby[0, pl.ds(x, 1), :] = fresh[0][0:1, :]
                    sby[1, pl.ds(x, 1), :] = fresh[2][0:1, :]
            return 0

        lax.fori_loop(0, blocks, run, 0)

    def fix_h_side(part, side_y, side_z):
        scale = cs_right[part]
        amount = take[0, last_x, part]
        hf[1, depth_x, part] = hf[1, depth_x, part] + scale * side_z
        hf[2, depth_x, part] = hf[2, depth_x, part] - scale * side_y
        me[3, last_x, part] = me[3, last_x, part] + amount * side_z
        me[4, last_x, part] = me[4, last_x, part] + amount * side_y

    def fix_e_side(part, side_y, side_z):
        scale = cs_left[part]
        amount = take[0, 0, part]
        ef[1, 0, part] = ef[1, 0, part] + scale * side_z
        ef[2, 0, part] = ef[2, 0, part] - scale * side_y
        mh[3, 0, part] = mh[3, 0, part] - amount * side_z
        mh[4, 0, part] = mh[4, 0, part] - amount * side_y

    ey_corner, hx_corner, ez_edge, ex_corner, hz_edge = (pl.ds(8 * n, 1) for n in range(5))
    rows_x, rows_y = pl.ds(0, depth_x), pl.ds(0, depth_y)

    def settle_e_low(step):
        arrived(step, "ay", "d1", "axl")
        slot = lax.rem(step, SLOTS)
        scale = cr_up[rows_x]
        below_x = ray[slot, 0] - scale * save_row_e[1]
        below_z = ray[slot, 1] + scale * save_row_e[0]
        row_h[0] = below_x
        row_h[1] = below_z
        row_h[1, last_x:depth_x, :] = (
            row_h[1, last_x:depth_x, :] - cr_up[depth_x:depth_x + 1, :] * rd1[slot, 1:2, :])
        scale = cr_right[low]
        side_y = raxl[slot, 0] + scale * save_e_lo[1]
        side_z = raxl[slot, 1] - scale * save_e_lo[0]
        lines[hx_corner] = rd1[slot, 0:1, :] - cr_d1[0:1, :] * lines[ez_edge]
        fix_e_side(low, side_y, side_z)
        for x in range(depth_x):
            line_hx, line_hz = row_h[0, x:x + 1, :], row_h[1, x:x + 1, :]
            amount, scale = edge_et[x], edge_e[x]
            ef[0, x, low] = ef[0, x, low] - scale * line_hz
            ef[2, x, low] = ef[2, x, low] + scale * line_hx
            mh[0, x, low] = mh[0, x, low] - amount * line_hz
            mh[5, x, low] = mh[5, x, low] - amount * line_hx
        scale = cs_down[rows_x]
        save_row_e[0] = sby[0] - scale * row_h[1]
        save_row_e[1] = sby[1] + scale * row_h[0]
        save_row_e[1, 0:1, :] = save_row_e[1, 0:1, :] - cs_down[depth_x:depth_x + 1, :] * side_y[0:1, :]
        save_e_lo[0] = ef[1, 0, low]
        save_e_lo[1] = ef[2, 0, low]

    def settle_h_low(step):
        arrived(step, "bxl")
        slot = lax.rem(step, SLOTS)
        scale = cr_left[low]
        side_y = rbxl[slot, 0] + scale * save_h_lo[1]
        side_z = rbxl[slot, 1] - scale * save_h_lo[0]
        corner = cr_left[depth_y:depth_y + 1, :] * lines[hx_corner]
        side_z = side_z + jnp.where(is_bottom, corner, 0.0)
        lines[ez_edge] = side_z[0:1, :]
        fix_h_side(low, side_y, side_z)
        save_h_lo[0] = hf[1, depth_x, low]
        save_h_lo[1] = hf[2, depth_x, low]
        sd2[0:1, :] = hf[1, depth_x, 0:1, :]

    def settle_h_high(step):
        arrived(step, "by", "d2", "bxh")
        slot = lax.rem(step, SLOTS)
        scale = cr_down[rows_x]
        row_e[0] = rby[slot, 0] - scale * save_row_h[1]
        row_e[1] = rby[slot, 1] + scale * save_row_h[0]
        row_e[1, 0:1, :] = row_e[1, 0:1, :] - cr_down[depth_x:depth_x + 1, :] * rd2[slot, 0:1, :]
        scale = cr_left[high]
        side_y = rbxh[slot, 0] + scale * save_h_hi[1]
        side_z = rbxh[slot, 1] - scale * save_h_hi[0]
        lines[ex_corner] = rd2[slot, 1:2, :] - cr_d2[0:1, :] * lines[hz_edge]
        fix_h_side(high, side_y, side_z)
        for x in range(depth_x):
            line_ex, line_ez = row_e[0, x:x + 1, :], row_e[1, x:x + 1, :]
            amount, scale = edge_ht[x], edge_h[x]
            hf[0, x + 1, high] = hf[0, x + 1, high] - scale * line_ez
            hf[2, x + 1, high] = hf[2, x + 1, high] + scale * line_ex
            me[0, x, high] = me[0, x, high] + amount * line_ez
            me[5, x, high] = me[5, x, high] + amount * line_ex
        scale = cs_up[rows_x]
        save_row_h[0] = say[0] - scale * row_e[1]
        save_row_h[1] = say[1] + scale * row_e[0]
        save_row_h[1, last_x:depth_x, :] = (
            save_row_h[1, last_x:depth_x, :] - cs_up[depth_x:depth_x + 1, :] * side_y[half - 1:half, :])
        save_h_hi[0] = hf[1, depth_x, high]
        save_h_hi[1] = hf[2, depth_x, high]

    def settle_e_high(step):
        arrived(step, "axh")
        slot = lax.rem(step, SLOTS)
        scale = cr_right[high]
        side_y = raxh[slot, 0] + scale * save_e_hi[1]
        side_z = raxh[slot, 1] - scale * save_e_hi[0]
        corner = cr_right[depth_y:depth_y + 1, :] * lines[ex_corner]
        side_z = side_z + jnp.where(is_top, corner, 0.0)
        lines[hz_edge] = side_z[half - 1:half, :]
        fix_e_side(high, side_y, side_z)
        save_e_hi[0] = ef[1, 0, high]
        save_e_hi[1] = ef[2, 0, high]

    def inject(step):
        top, rest = split_two(courant * current[pl.ds(step, 1), :])
        total = None
        for part in (top, rest):
            piece = jnp.dot(
                cell_t[...] * part, depth[...], preferred_element_type=jnp.float32
            )
            total = piece if total is None else total + piece
        source[...] = total.reshape(source.shape)

    def read_out(values, step):
        top, rest = split_two(values.reshape(depth_x * depth_y, depth_z))
        picked = jnp.dot(top, depth_t[...], preferred_element_type=jnp.float32)
        picked = picked + jnp.dot(rest, depth_t[...], preferred_element_type=jnp.float32)
        chosen = jnp.sum(picked * cell_f[...], axis=0, keepdims=True)
        record[pl.ds(step, 1), :] = chosen * current[pl.ds(step, 1), :]

    pl.semaphore_wait(barrier, len(line_x) + len(line_y) + len(across))
    for wanted, _, copy in once:
        pl.when(wanted)(copy.start)
    for copy in loads:
        copy.wait()

    for x in range(depth_x):
        sby[0, x:x + 1, :] = ef[0, x, 0:1, :]
        sby[1, x:x + 1, :] = ef[2, x, 0:1, :]
    for c in (1, 2):
        sbxl[c - 1] = ef[c, 0, low]
        sbxh[c - 1] = ef[c, 0, high]
    sd2[1:2, :] = ef[0, last_x, 0:1, :]
    send(0, "by", "bxl", "bxh", "d2")
    save_row_e[...] = sby[...]
    save_e_lo[...] = sbxl[...]
    save_e_hi[...] = sbxh[...]

    cells = (cell_ref[0:1, :] - ix * depth_x) * depth_y + (cell_ref[1:2, :] - iy * depth_y)
    hit = lax.broadcasted_iota(jnp.int32, cell_f.shape, 0) == cells
    cell_f[...] = jnp.where(hit, 1.0, 0.0)
    cell_t[...] = jnp.where(hit, 1.0, 0.0).astype(jnp.bfloat16)
    hit = lax.broadcasted_iota(jnp.int32, depth_t.shape, 0) == cell_ref[2:3, :]
    table = jnp.where(hit, 1.0, 0.0)
    depth_t[...] = table.astype(jnp.bfloat16)
    depth[...] = table.T.astype(jnp.bfloat16)
    live = lax.broadcasted_iota(jnp.int32, (1, slots), 1) < live_ref[0]
    flow = lax.dot_general(
        wave_ref[...], inj_ref[...], (((1,), (1,)), ((), ())), preferred_element_type=jnp.float32
    )
    current[...] = jnp.where(live, flow, 0.0)
    for wanted, expected, copy in once:
        pl.when(wanted)(copy.wait_send)
        pl.when(expected)(copy.wait_recv)

    def turn(step, _):
        more = step < steps
        update_h(True)
        for c in (1, 2):
            saxh[c - 1] = hf[c, depth_x, high]
        sd1[0:1, :] = say[0, 0:1, :]
        sd1[1:2, :] = ef[1, 0, last_y:depth_y, :]
        send(step, "d1", "ay", "axh")
        inject(step - 1)
        pl.when(step > 1)(lambda: settle_e_low(step - 1))
        update_h(False)
        for c in (1, 2):
            saxl[c - 1] = hf[c, depth_x, low]
        send(step, "axl")
        sent(step - 1, "by", "bxl", "d2")
        settle_h_low(step - 1)
        update_e(False)
        for c in (1, 2):
            sbxl[c - 1] = ef[c, 0, low]
        sd2[1:2, :] = sby[0, last_x:depth_x, :]
        pl.when(more)(lambda: send(step, "d2", "by", "bxl"))
        read_out(z_copy[...], lax.rem(step + steps - 2, steps))
        sent(step - 1, "bxh")
        settle_h_high(step - 1)
        update_e(True)
        for c in (1, 2):
            sbxh[c - 1] = ef[c, 0, high]
        pl.when(more)(lambda: send(step, "bxh"))
        sent(step, "ay", "axh", "d1", "axl")
        settle_e_high(step)
        return 0

    lax.fori_loop(1, steps + 1, turn, 0)
    settle_e_low(steps)
    stores = [
        pltpu.make_async_copy(ef.at[:, pl.ds(0, depth_x)], e_out, store_sem.at[0]),
        pltpu.make_async_copy(hf.at[:, pl.ds(1, depth_x)], h_out, store_sem.at[1]),
    ]
    for copy in stores:
        copy.start()
    read_out(ef[2, pl.ds(0, depth_x)], steps - 1)
    member = lax.broadcasted_iota(jnp.int32, (ports, slots), 0) == port_ref[...]
    member = jnp.where(member, 1.0, 0.0).astype(jnp.bfloat16)
    total = None
    for part in split_two(record[...]):
        piece = lax.dot_general(
            part, member, (((1,), (1,)), ((), ())), preferred_element_type=jnp.float32
        )
        total = piece if total is None else total + piece
    for row in range(steps):
        share[row] = total[row:row + 1, :]
    chunk = steps // count_y

    def spread(first, peers, source_of, target):
        moves = []
        for number, peer in enumerate(peers):
            moves.append(pltpu.make_async_remote_copy(
                src_ref=source_of(peer), dst_ref=target,
                send_sem=send_sum.at[first + number], recv_sem=recv_sum.at[first + number],
                device_id=peer, device_id_type=MESH))
            moves[-1].start()
        return moves

    def settle(moves):
        for move in moves:
            move.wait()

    mine = pl.ds(iy * chunk, chunk)
    moves = spread(
        0, line_y, lambda peer: share.at[pl.ds(peer[1] * chunk, chunk)], from_y.at[iy]
    )
    from_y[iy] = share[mine]
    settle(moves)
    from_x[ix] = sum(from_y[j] for j in range(count_y))
    first = len(line_y)
    settle(spread(first, line_x, lambda peer: from_x.at[ix], from_x.at[ix]))
    result[mine] = sum(from_x[i] for i in range(count_x))
    first = first + len(line_x)
    settle(spread(first, line_y, lambda peer: result.at[mine], result.at[mine]))
    for row in range(steps):
        power_ref[row:row + 1, :] = result[row]
    for copy in stores:
        copy.wait()


def local(
    electric, magnetic, aux_electric, aux_magnetic, grades, permittivity,
    dipole_cell, dipole_port, live_count, injection, waveform,
):
    depth_x, depth_y, depth_z = permittivity.shape
    slots = dipole_cell.shape[1]
    ports, steps = waveform.shape
    block = (depth_x, depth_y, depth_z)
    cells = depth_x * depth_y
    f32 = jnp.float32
    count_x, count_y = lax.axis_size("gx"), lax.axis_size("gy")
    chunk = steps // count_y
    assert chunk * count_y == steps
    transfers = count_x + 2 * count_y
    half = depth_y // 2
    row = (2, depth_x, depth_z)
    side = (2, half, depth_z)
    pair = (2, depth_z)
    messages = (row, row, side, side, side, side, pair, pair)
    tall, wide, single = (depth_x + 8, depth_z), (depth_y + 8, depth_z), (8, depth_z)
    coefficients = (tall, tall, wide, wide, single, single)
    shapes = (
        messages + tuple((SLOTS,) + shape for shape in messages) + coefficients + coefficients
        + (row,) * 4 + (side,) * 4 + ((40, depth_z),) + ((depth_x, half, depth_z),) * 4
    )
    scratch = [pltpu.VMEM(shape, f32) for shape in shapes]
    vmem = pl.BlockSpec(memory_space=pltpu.VMEM)
    anywhere = pl.BlockSpec(memory_space=pltpu.HBM)
    electric, magnetic, power = pl.pallas_call(
        kernel,
        out_shape=(
            jax.ShapeDtypeStruct(electric.shape, f32),
            jax.ShapeDtypeStruct(magnetic.shape, f32),
            jax.ShapeDtypeStruct((steps, ports), f32),
        ),
        in_specs=[anywhere] * 4 + [vmem] * 4
        + [pl.BlockSpec(memory_space=pltpu.SMEM)] + [vmem] * 2,
        out_specs=(anywhere, anywhere, vmem),
        scratch_shapes=[
            pltpu.VMEM((3, depth_x + 1, depth_y, depth_z), f32),
            pltpu.VMEM((3, depth_x + 1, depth_y, depth_z), f32),
            pltpu.VMEM((6,) + block, f32),
            pltpu.VMEM((6,) + block, f32),
            pltpu.VMEM((3,) + block, f32),
            pltpu.VMEM((3,) + block, f32),
            pltpu.VMEM(block, f32),
            pltpu.VMEM(block, f32),
            *scratch,
            pltpu.VMEM((cells, slots), jnp.bfloat16),
            pltpu.VMEM((cells, slots), f32),
            pltpu.VMEM((depth_z, slots), jnp.bfloat16),
            pltpu.VMEM((slots, depth_z), jnp.bfloat16),
            pltpu.VMEM((steps, slots), f32),
            pltpu.VMEM((steps, slots), f32),
            pltpu.VMEM(block, f32),
            pltpu.VMEM((steps, 1, ports), f32),
            pltpu.VMEM((count_y, chunk, 1, ports), f32),
            pltpu.VMEM((count_x, chunk, 1, ports), f32),
            pltpu.VMEM((steps, 1, ports), f32),
            pltpu.SemaphoreType.DMA((4,)),
            pltpu.SemaphoreType.DMA((2,)),
            pltpu.SemaphoreType.DMA((len(KINDS),)),
            pltpu.SemaphoreType.DMA((len(KINDS), SLOTS)),
            pltpu.SemaphoreType.DMA((len(COEFFICIENTS),)),
            pltpu.SemaphoreType.DMA((len(COEFFICIENTS),)),
            pltpu.SemaphoreType.DMA((transfers,)),
            pltpu.SemaphoreType.DMA((transfers,)),
        ],
        compiler_params=pltpu.CompilerParams(
            collective_id=0, has_side_effects=True, vmem_limit_bytes=60 * 1024 * 1024
        ),
    )(
        electric, magnetic, aux_electric, aux_magnetic, grades, permittivity,
        dipole_cell, dipole_port.reshape(1, slots), live_count, injection, waveform.T,
    )
    return electric, magnetic, power


def solution(mesh):
    in_specs = (
        P(None, "gx", "gy", None),
        P(None, "gx", "gy", None),
        P(None, "gx", "gy", None),
        P(None, "gx", "gy", None),
        P(None, "gx", "gy", None),
        P("gx", "gy", None),
        P(None, ("gx", "gy")),
        P(("gx", "gy")),
        P(("gx", "gy")),
        P(("gx", "gy"), None),
        P(),
    )
    out_specs = (P(None, "gx", "gy", None), P(None, "gx", "gy", None), P())
    return jax.shard_map(local, mesh=mesh, in_specs=in_specs, out_specs=out_specs, check_vma=False)
```

```python
import functools

import jax
import jax.numpy as jnp
from jax import lax
from jax.experimental import pallas as pl
from jax.experimental.pallas import tpu as pltpu
from jax.sharding import PartitionSpec as P

MESH = pl.DeviceIdType.MESH
courant = 0.55
absorb_keep = (0.0, 0.92, 0.75, 0.45)
absorb_take = (0.0, -0.06, -0.18, -0.35)
derivative_pairs = ((2, 1), (1, 2), (0, 2), (2, 0), (1, 0), (0, 1))
UNROLL = 8
TAIL = 4


def grade_table(grades, table):
    result = jnp.where(grades == 1, table[1], 0.0)
    result = jnp.where(grades == 2, table[2], result)
    return jnp.where(grades == 3, table[3], result)


def split_two(values):
    high = values.astype(jnp.bfloat16)
    low = (values - high.astype(jnp.float32)).astype(jnp.bfloat16)
    return high, low


KINDS = ("ay", "by", "axh", "axl", "bxl", "bxh", "d1", "d2")
TRAVEL = {
    "ay": (0, 1), "by": (0, -1), "axh": (1, 0), "axl": (1, 0),
    "bxl": (-1, 0), "bxh": (-1, 0), "d1": (-1, 1), "d2": (1, -1),
}
COEFFICIENTS = ((0, 1), (0, -1), (1, 0), (-1, 0), (-1, 1), (1, -1))
SLOTS = 4


def kernel(
    e_in, h_in, me_in, mh_in, grades_ref, eps_ref, cell_ref, port_ref, live_ref, inj_ref, wave_ref,
    e_out, h_out, power_ref,
    ef, hf, me, mh, grades, eps, inj, keep, take, factor, source, member,
    say, sby, saxh, saxl, sbxl, sbxh, sd1, sd2,
    ray, rby, raxh, raxl, rbxl, rbxh, rd1, rd2,
    cs_up, cs_down, cs_right, cs_left, cs_d1, cs_d2,
    cr_up, cr_down, cr_right, cr_left, cr_d1, cr_d2,
    row_h, row_e, save_row_h, save_row_e, save_h_lo, save_h_hi, save_e_lo, save_e_hi, lines,
    edge_h, edge_ht, edge_e, edge_et,
    cell_t, cell_f, depth_t, depth, current, record, z_copy,
    share, from_y, from_x, result, late, late_y, late_x,
    load_sem, store_sem, send_sem, recv_sem, send_one, recv_one, send_sum, recv_sum, send_late, recv_late,
):
    depth_x, depth_y, depth_z = eps_ref.shape
    ports, slots = inj_ref.shape[1], inj_ref.shape[0]
    steps = wave_ref.shape[0]
    half = depth_y // 2
    last_x, last_y = depth_x - 1, depth_y - 1
    ix, iy = lax.axis_index("gx"), lax.axis_index("gy")
    count_x, count_y = lax.axis_size("gx"), lax.axis_size("gy")
    f32 = jnp.float32

    def there(dx, dy):
        found = ix >= 0
        if dx:
            found = jnp.logical_and(found, ix > 0 if dx < 0 else ix < count_x - 1)
        if dy:
            found = jnp.logical_and(found, iy > 0 if dy < 0 else iy < count_y - 1)
        return found

    loads = [
        pltpu.make_async_copy(grades_ref, grades, load_sem.at[4]),
        pltpu.make_async_copy(eps_ref, eps, load_sem.at[5]),
        pltpu.make_async_copy(e_in, ef.at[:, pl.ds(0, depth_x)], load_sem.at[0]),
        pltpu.make_async_copy(h_in, hf.at[:, pl.ds(1, depth_x)], load_sem.at[1]),
        pltpu.make_async_copy(me_in, me, load_sem.at[2]),
        pltpu.make_async_copy(mh_in, mh, load_sem.at[3]),
        pltpu.make_async_copy(inj_ref, inj, load_sem.at[6]),
    ]
    for copy in loads:
        copy.start()
    record[...] = jnp.zeros(record.shape, f32)

    plane = jnp.zeros((depth_y, depth_z), f32)
    for component in range(3):
        ef[component, depth_x] = plane
        hf[component, 0] = plane
    for ref in (
        ray, rby, raxh, raxl, rbxl, rbxh, rd1, rd2,
        cr_up, cr_down, cr_right, cr_left, cr_d1, cr_d2,
        save_row_h, save_h_lo, save_h_hi, lines, sd2, cs_up, cs_down, cs_right, cs_left, cs_d1, cs_d2,
    ):
        ref[...] = jnp.zeros(ref.shape, f32)

    barrier = pltpu.get_barrier_semaphore()
    line_x = [(lax.rem(ix + offset, count_x), iy) for offset in range(1, count_x)]
    line_y = [(ix, lax.rem(iy + offset, count_y)) for offset in range(1, count_y)]
    across = [
        (lax.rem(ix + count_x - 1, count_x), lax.rem(iy + 1, count_y)),
        (lax.rem(ix + 1, count_x), lax.rem(iy + count_y - 1, count_y)),
    ]
    for peer in line_x + line_y + across:
        pl.semaphore_signal(barrier, inc=1, device_id=peer, device_id_type=MESH)

    def prepare(x, _):
        for d in range(3):
            level = grades[d, x]
            keep[d, x] = grade_table(level, absorb_keep)
            take[d, x] = grade_table(level, absorb_take)
        factor[x] = courant / eps[x]
        return 0

    for copy in loads[:2]:
        copy.wait()
    lax.fori_loop(0, depth_x, prepare, 0)

    row_half = lax.broadcasted_iota(jnp.int32, (half, depth_z), 0)
    is_top, is_bottom = row_half == half - 1, row_half == 0

    for x in range(depth_x):
        upper = take[1, x, half:, :]
        lower = take[1, x, :half, :]
        scale_h = courant * (1.0 + upper)
        scale_e = factor[x, :half, :] * (1.0 + lower)
        edge_h[x] = jnp.where(is_top, scale_h, 0.0)
        edge_ht[x] = jnp.where(is_top, upper, 0.0)
        edge_e[x] = jnp.where(is_bottom, scale_e, 0.0)
        edge_et[x] = jnp.where(is_bottom, lower, 0.0)
        cs_up[x:x + 1, :] = scale_h[half - 1:half, :]
        cs_down[x:x + 1, :] = scale_e[0:1, :]
    cs_right[0:depth_y, :] = courant * (1.0 + take[0, last_x])
    cs_left[0:depth_y, :] = factor[0] * (1.0 + take[0, 0])
    cs_up[depth_x:depth_x + 1, :] = cs_right[last_y:depth_y, :]
    cs_down[depth_x:depth_x + 1, :] = cs_left[0:1, :]
    cs_right[depth_y:depth_y + 1, :] = cs_up[last_x:depth_x, :]
    cs_left[depth_y:depth_y + 1, :] = cs_down[0:1, :]
    cs_d1[0:1, :] = cs_up[0:1, :]
    cs_d2[0:1, :] = cs_down[last_x:depth_x, :]

    once = []
    for number, (source_ref, target_ref) in enumerate((
        (cs_up, cr_up), (cs_down, cr_down), (cs_right, cr_right),
        (cs_left, cr_left), (cs_d1, cr_d1), (cs_d2, cr_d2),
    )):
        dx, dy = COEFFICIENTS[number]
        once.append((there(dx, dy), there(-dx, -dy), pltpu.make_async_remote_copy(
            src_ref=source_ref, dst_ref=target_ref,
            send_sem=send_one.at[number], recv_sem=recv_one.at[number],
            device_id=(ix + dx, iy + dy), device_id_type=MESH)))

    sends = dict(ay=say, by=sby, axh=saxh, axl=saxl, bxl=sbxl, bxh=sbxh, d1=sd1, d2=sd2)
    gets = dict(ay=ray, by=rby, axh=raxh, axl=raxl, bxl=rbxl, bxh=rbxh, d1=rd1, d2=rd2)

    def message(kind, step):
        number = KINDS.index(kind)
        slot = lax.rem(step, SLOTS)
        dx, dy = TRAVEL[kind]
        return pltpu.make_async_remote_copy(
            src_ref=sends[kind], dst_ref=gets[kind].at[slot],
            send_sem=send_sem.at[number], recv_sem=recv_sem.at[number, slot],
            device_id=(ix + dx, iy + dy), device_id_type=MESH)

    def send(step, *kinds):
        for kind in kinds:
            dx, dy = TRAVEL[kind]
            pl.when(there(dx, dy))(message(kind, step).start)

    def sent(step, *kinds):
        for kind in kinds:
            dx, dy = TRAVEL[kind]
            pl.when(there(dx, dy))(message(kind, step).wait_send)

    def arrived(step, *kinds):
        for kind in kinds:
            dx, dy = TRAVEL[kind]
            pl.when(there(-dx, -dy))(message(kind, step).wait_recv)

    low, high = slice(0, half), slice(half, depth_y)
    lanes = lax.broadcasted_iota(jnp.int32, (half, depth_z), 1)
    z_last, z_first = lanes == depth_z - 1, lanes == 0

    def curl(x, part, here, beside, line, memory, forward):
        turn_y = half - 1 if forward else 1
        turn_z = depth_z - 1 if forward else 1
        edge_y = is_top if forward else is_bottom
        edge_z = z_last if forward else z_first
        terms = []
        for number, (component, axis) in enumerate(derivative_pairs):
            value = here[component]
            if axis == 0:
                other = beside[component]
            elif axis == 1:
                other = jnp.where(edge_y, line[component], pltpu.roll(value, turn_y, 0))
            else:
                other = jnp.where(edge_z, 0.0, pltpu.roll(value, turn_z, 1))
            slope = other - value if forward else value - other
            carried = keep[axis, x, part] * memory[number, x, part] + take[axis, x, part] * slope
            memory[number, x, part] = carried
            terms.append(slope + carried)
        return (terms[0] - terms[1], terms[2] - terms[3], terms[4] - terms[5])

    blocks = depth_x // UNROLL
    no_line = [0.0, None, 0.0]

    def update_h(upper):
        part = high if upper else low

        def run(block, _):
            for inner in range(UNROLL):
                x = block * UNROLL + inner
                here = [ef[c, x, part] for c in range(3)]
                beside = [None, ef[1, x + 1, part], ef[2, x + 1, part]]
                line = no_line
                if not upper:
                    line = [ef[0, x, half:half + 1, :], None, ef[2, x, half:half + 1, :]]
                rotation = curl(x, part, here, beside, line, me, True)
                fresh = [hf[c, x + 1, part] - courant * rotation[c] for c in range(3)]
                for c in range(3):
                    hf[c, x + 1, part] = fresh[c]
                z_copy[x, part] = here[2]
                if upper:
                    say[0, pl.ds(x, 1), :] = fresh[0][half - 1:half, :]
                    say[1, pl.ds(x, 1), :] = fresh[2][half - 1:half, :]
            return 0

        lax.fori_loop(0, blocks, run, 0)

    def update_e(upper):
        part = high if upper else low

        def run(block, _):
            for inner in range(UNROLL):
                x = block * UNROLL + inner
                here = [hf[c, x + 1, part] for c in range(3)]
                beside = [None, hf[1, x, part], hf[2, x, part]]
                line = no_line
                if upper:
                    line = [hf[0, x + 1, half - 1:half, :], None, hf[2, x + 1, half - 1:half, :]]
                rotation = curl(x, part, here, beside, line, mh, False)
                ratio = factor[x, part]
                fresh = [ef[c, x, part] + ratio * rotation[c] for c in range(3)]
                fresh[2] = fresh[2] - source[x, part]
                for c in range(3):
                    ef[c, x, part] = fresh[c]
                if not upper:
                    sby[0, pl.ds(x, 1), :] = fresh[0][0:1, :]
                    sby[1, pl.ds(x, 1), :] = fresh[2][0:1, :]
            return 0

        lax.fori_loop(0, blocks, run, 0)

    def fix_h_side(part, side_y, side_z):
        scale = cs_right[part]
        amount = take[0, last_x, part]
        hf[1, depth_x, part] = hf[1, depth_x, part] + scale * side_z
        hf[2, depth_x, part] = hf[2, depth_x, part] - scale * side_y
        me[3, last_x, part] = me[3, last_x, part] + amount * side_z
        me[4, last_x, part] = me[4, last_x, part] + amount * side_y

    def fix_e_side(part, side_y, side_z):
        scale = cs_left[part]
        amount = take[0, 0, part]
        ef[1, 0, part] = ef[1, 0, part] + scale * side_z
        ef[2, 0, part] = ef[2, 0, part] - scale * side_y
        mh[3, 0, part] = mh[3, 0, part] - amount * side_z
        mh[4, 0, part] = mh[4, 0, part] - amount * side_y

    ey_corner, hx_corner, ez_edge, ex_corner, hz_edge = (pl.ds(8 * n, 1) for n in range(5))
    rows_x, rows_y = pl.ds(0, depth_x), pl.ds(0, depth_y)

    def settle_e_low(step):
        arrived(step, "ay", "d1", "axl")
        slot = lax.rem(step, SLOTS)
        scale = cr_up[rows_x]
        below_x = ray[slot, 0] - scale * save_row_e[1]
        below_z = ray[slot, 1] + scale * save_row_e[0]
        row_h[0] = below_x
        row_h[1] = below_z
        row_h[1, last_x:depth_x, :] = (
            row_h[1, last_x:depth_x, :] - cr_up[depth_x:depth_x + 1, :] * rd1[slot, 1:2, :])
        scale = cr_right[low]
        side_y = raxl[slot, 0] + scale * save_e_lo[1]
        side_z = raxl[slot, 1] - scale * save_e_lo[0]
        lines[hx_corner] = rd1[slot, 0:1, :] - cr_d1[0:1, :] * lines[ez_edge]
        fix_e_side(low, side_y, side_z)
        for x in range(depth_x):
            line_hx, line_hz = row_h[0, x:x + 1, :], row_h[1, x:x + 1, :]
            amount, scale = edge_et[x], edge_e[x]
            ef[0, x, low] = ef[0, x, low] - scale * line_hz
            ef[2, x, low] = ef[2, x, low] + scale * line_hx
            mh[0, x, low] = mh[0, x, low] - amount * line_hz
            mh[5, x, low] = mh[5, x, low] - amount * line_hx
        scale = cs_down[rows_x]
        save_row_e[0] = sby[0] - scale * row_h[1]
        save_row_e[1] = sby[1] + scale * row_h[0]
        save_row_e[1, 0:1, :] = save_row_e[1, 0:1, :] - cs_down[depth_x:depth_x + 1, :] * side_y[0:1, :]
        save_e_lo[0] = ef[1, 0, low]
        save_e_lo[1] = ef[2, 0, low]

    def settle_h_low(step):
        arrived(step, "bxl")
        slot = lax.rem(step, SLOTS)
        scale = cr_left[low]
        side_y = rbxl[slot, 0] + scale * save_h_lo[1]
        side_z = rbxl[slot, 1] - scale * save_h_lo[0]
        corner = cr_left[depth_y:depth_y + 1, :] * lines[hx_corner]
        side_z = side_z + jnp.where(is_bottom, corner, 0.0)
        lines[ez_edge] = side_z[0:1, :]
        fix_h_side(low, side_y, side_z)
        save_h_lo[0] = hf[1, depth_x, low]
        save_h_lo[1] = hf[2, depth_x, low]
        sd2[0:1, :] = hf[1, depth_x, 0:1, :]

    def settle_h_high(step):
        arrived(step, "by", "d2", "bxh")
        slot = lax.rem(step, SLOTS)
        scale = cr_down[rows_x]
        row_e[0] = rby[slot, 0] - scale * save_row_h[1]
        row_e[1] = rby[slot, 1] + scale * save_row_h[0]
        row_e[1, 0:1, :] = row_e[1, 0:1, :] - cr_down[depth_x:depth_x + 1, :] * rd2[slot, 0:1, :]
        scale = cr_left[high]
        side_y = rbxh[slot, 0] + scale * save_h_hi[1]
        side_z = rbxh[slot, 1] - scale * save_h_hi[0]
        lines[ex_corner] = rd2[slot, 1:2, :] - cr_d2[0:1, :] * lines[hz_edge]
        fix_h_side(high, side_y, side_z)
        for x in range(depth_x):
            line_ex, line_ez = row_e[0, x:x + 1, :], row_e[1, x:x + 1, :]
            amount, scale = edge_ht[x], edge_h[x]
            hf[0, x + 1, high] = hf[0, x + 1, high] - scale * line_ez
            hf[2, x + 1, high] = hf[2, x + 1, high] + scale * line_ex
            me[0, x, high] = me[0, x, high] + amount * line_ez
            me[5, x, high] = me[5, x, high] + amount * line_ex
        scale = cs_up[rows_x]
        save_row_h[0] = say[0] - scale * row_e[1]
        save_row_h[1] = say[1] + scale * row_e[0]
        save_row_h[1, last_x:depth_x, :] = (
            save_row_h[1, last_x:depth_x, :] - cs_up[depth_x:depth_x + 1, :] * side_y[half - 1:half, :])
        save_h_hi[0] = hf[1, depth_x, high]
        save_h_hi[1] = hf[2, depth_x, high]

    def settle_e_high(step):
        arrived(step, "axh")
        slot = lax.rem(step, SLOTS)
        scale = cr_right[high]
        side_y = raxh[slot, 0] + scale * save_e_hi[1]
        side_z = raxh[slot, 1] - scale * save_e_hi[0]
        corner = cr_right[depth_y:depth_y + 1, :] * lines[ex_corner]
        side_z = side_z + jnp.where(is_top, corner, 0.0)
        lines[hz_edge] = side_z[half - 1:half, :]
        fix_e_side(high, side_y, side_z)
        save_e_hi[0] = ef[1, 0, high]
        save_e_hi[1] = ef[2, 0, high]

    def inject(step):
        top, rest = split_two(courant * current[pl.ds(step, 1), :])
        total = None
        for part in (top, rest):
            piece = jnp.dot(
                cell_t[...] * part, depth[...], preferred_element_type=jnp.float32
            )
            total = piece if total is None else total + piece
        source[...] = total.reshape(source.shape)

    def read_out(values, step):
        top, rest = split_two(values.reshape(depth_x * depth_y, depth_z))
        picked = jnp.dot(top, depth_t[...], preferred_element_type=jnp.float32)
        picked = picked + jnp.dot(rest, depth_t[...], preferred_element_type=jnp.float32)
        chosen = jnp.sum(picked * cell_f[...], axis=0, keepdims=True)
        record[pl.ds(step, 1), :] = chosen * current[pl.ds(step, 1), :]

    cells = (cell_ref[0:1, :] - ix * depth_x) * depth_y + (cell_ref[1:2, :] - iy * depth_y)
    hit = lax.broadcasted_iota(jnp.int32, cell_f.shape, 0) == cells
    cell_f[...] = jnp.where(hit, 1.0, 0.0)
    cell_t[...] = jnp.where(hit, 1.0, 0.0).astype(jnp.bfloat16)
    hit = lax.broadcasted_iota(jnp.int32, depth_t.shape, 0) == cell_ref[2:3, :]
    table = jnp.where(hit, 1.0, 0.0)
    depth_t[...] = table.astype(jnp.bfloat16)
    depth[...] = table.T.astype(jnp.bfloat16)
    live = lax.broadcasted_iota(jnp.int32, (1, slots), 1) < live_ref[0]
    loads[6].wait()
    flow = lax.dot_general(
        wave_ref[...], inj[...], (((1,), (1,)), ((), ())), preferred_element_type=jnp.float32
    )
    current[...] = jnp.where(live, flow, 0.0)
    hit = lax.broadcasted_iota(jnp.int32, (ports, slots), 0) == port_ref[...]
    member[...] = jnp.where(hit, 1.0, 0.0).astype(jnp.bfloat16)
    for copy in loads[2:6]:
        copy.wait()

    for x in range(depth_x):
        sby[0, x:x + 1, :] = ef[0, x, 0:1, :]
        sby[1, x:x + 1, :] = ef[2, x, 0:1, :]
    for c in (1, 2):
        sbxl[c - 1] = ef[c, 0, low]
        sbxh[c - 1] = ef[c, 0, high]
    sd2[1:2, :] = ef[0, last_x, 0:1, :]
    pl.semaphore_wait(barrier, len(line_x) + len(line_y) + len(across))
    for wanted, _, copy in once:
        pl.when(wanted)(copy.start)
    send(0, "by", "bxl", "bxh", "d2")
    save_row_e[...] = sby[...]
    save_e_lo[...] = sbxl[...]
    save_e_hi[...] = sbxh[...]


    def port_sums():
        total = None
        for part in split_two(record[...]):
            piece = lax.dot_general(
                part, member[...], (((1,), (1,)), ((), ())), preferred_element_type=f32
            )
            total = piece if total is None else total + piece
        return total

    chunk = steps // count_y
    mine = pl.ds(iy * chunk, chunk)

    def spread(sems, first, peers, source_of, target):
        return [
            pltpu.make_async_remote_copy(
                src_ref=source_of(peer), dst_ref=target,
                send_sem=sems[0].at[first + number], recv_sem=sems[1].at[first + number],
                device_id=peer, device_id_type=MESH)
            for number, peer in enumerate(peers)
        ]

    def launch(moves):
        for move in moves:
            move.start()

    def settle(moves):
        for move in moves:
            move.wait()

    sums = (send_sum, recv_sum)

    def first_moves():
        return spread(
            sums, 0, line_y, lambda peer: share.at[pl.ds(peer[1] * chunk, chunk)], from_y.at[iy])

    def second_moves():
        return spread(sums, len(line_y), line_x, lambda peer: from_x.at[ix], from_x.at[ix])

    def third_moves():
        first = len(line_y) + len(line_x)
        return spread(sums, first, line_y, lambda peer: result.at[mine], result.at[mine])

    def reduce_one():
        total = port_sums()
        for row in range(steps):
            share[row] = total[row:row + 1, :]
        launch(first_moves())
        from_y[iy] = share[mine]

    def reduce_two():
        settle(first_moves())
        from_x[ix] = sum(from_y[j] for j in range(count_y))
        launch(second_moves())

    def reduce_three():
        settle(second_moves())
        result[mine] = sum(from_x[i] for i in range(count_x))
        launch(third_moves())

    def turn(step, _):
        more = step < steps
        update_h(True)
        for c in (1, 2):
            saxh[c - 1] = hf[c, depth_x, high]
        sd1[0:1, :] = say[0, 0:1, :]
        sd1[1:2, :] = ef[1, 0, last_y:depth_y, :]
        send(step, "d1", "ay", "axh")
        inject(step - 1)
        pl.when(step > 1)(lambda: settle_e_low(step - 1))
        update_h(False)
        for c in (1, 2):
            saxl[c - 1] = hf[c, depth_x, low]
        send(step, "axl")
        sent(step - 1, "by", "bxl", "d2")

        @pl.when(step == 1)
        def _():
            for wanted, expected, copy in once:
                pl.when(wanted)(copy.wait_send)
                pl.when(expected)(copy.wait_recv)

        settle_h_low(step - 1)
        update_e(False)
        for c in (1, 2):
            sbxl[c - 1] = ef[c, 0, low]
        sd2[1:2, :] = sby[0, last_x:depth_x, :]
        pl.when(more)(lambda: send(step, "d2", "by", "bxl"))
        read_out(z_copy[...], lax.rem(step + steps - 2, steps))
        pl.when(step == steps - TAIL + 1)(reduce_one)
        pl.when(step == steps - TAIL + 3)(reduce_two)
        pl.when(step == steps - TAIL + 4)(reduce_three)
        sent(step - 1, "bxh")
        settle_h_high(step - 1)
        update_e(True)
        for c in (1, 2):
            sbxh[c - 1] = ef[c, 0, high]
        pl.when(more)(lambda: send(step, "bxh"))
        sent(step, "ay", "axh", "d1", "axl")
        settle_e_high(step)
        return 0

    lax.fori_loop(1, steps + 1, turn, 0)
    settle_e_low(steps)
    stores = [
        pltpu.make_async_copy(ef.at[:, pl.ds(0, depth_x)], e_out, store_sem.at[0]),
        pltpu.make_async_copy(hf.at[:, pl.ds(1, depth_x)], h_out, store_sem.at[1]),
    ]
    for copy in stores:
        copy.start()
    read_out(ef[2, pl.ds(0, depth_x)], steps - 1)
    late[...] = port_sums()[steps - TAIL:, :]
    lates = (send_late, recv_late)
    moves = spread(lates, 0, line_y, lambda peer: late, late_y.at[iy])
    launch(moves)
    late_y[iy] = late[...]
    settle(third_moves())
    for row in range(steps - TAIL):
        power_ref[row:row + 1, :] = result[row]
    settle(moves)
    late_x[ix] = sum(late_y[j] for j in range(count_y))
    moves = spread(lates, len(line_y), line_x, lambda peer: late_x.at[ix], late_x.at[ix])
    launch(moves)
    settle(moves)
    power_ref[steps - TAIL:, :] = sum(late_x[i] for i in range(count_x))
    for copy in stores:
        copy.wait()


def local(
    electric, magnetic, aux_electric, aux_magnetic, grades, permittivity,
    dipole_cell, dipole_port, live_count, injection, waveform,
):
    depth_x, depth_y, depth_z = permittivity.shape
    slots = dipole_cell.shape[1]
    ports, steps = waveform.shape
    block = (depth_x, depth_y, depth_z)
    cells = depth_x * depth_y
    f32 = jnp.float32
    count_x, count_y = lax.axis_size("gx"), lax.axis_size("gy")
    chunk = steps // count_y
    assert chunk * count_y == steps
    transfers = count_x + 2 * count_y
    half = depth_y // 2
    row = (2, depth_x, depth_z)
    side = (2, half, depth_z)
    pair = (2, depth_z)
    messages = (row, row, side, side, side, side, pair, pair)
    tall, wide, single = (depth_x + 8, depth_z), (depth_y + 8, depth_z), (8, depth_z)
    coefficients = (tall, tall, wide, wide, single, single)
    shapes = (
        messages + tuple((SLOTS,) + shape for shape in messages) + coefficients + coefficients
        + (row,) * 4 + (side,) * 4 + ((40, depth_z),) + ((depth_x, half, depth_z),) * 4
    )
    scratch = [pltpu.VMEM(shape, f32) for shape in shapes]
    vmem = pl.BlockSpec(memory_space=pltpu.VMEM)
    anywhere = pl.BlockSpec(memory_space=pltpu.HBM)
    electric, magnetic, power = pl.pallas_call(
        kernel,
        out_shape=(
            jax.ShapeDtypeStruct(electric.shape, f32),
            jax.ShapeDtypeStruct(magnetic.shape, f32),
            jax.ShapeDtypeStruct((steps, ports), f32),
        ),
        in_specs=[anywhere] * 6 + [vmem] * 2
        + [pl.BlockSpec(memory_space=pltpu.SMEM), anywhere, vmem],
        out_specs=(anywhere, anywhere, vmem),
        scratch_shapes=[
            pltpu.VMEM((3, depth_x + 1, depth_y, depth_z), f32),
            pltpu.VMEM((3, depth_x + 1, depth_y, depth_z), f32),
            pltpu.VMEM((6,) + block, f32),
            pltpu.VMEM((6,) + block, f32),
            pltpu.VMEM((3,) + block, jnp.int32),
            pltpu.VMEM(block, f32),
            pltpu.VMEM((slots, ports), jnp.bfloat16),
            pltpu.VMEM((3,) + block, f32),
            pltpu.VMEM((3,) + block, f32),
            pltpu.VMEM(block, f32),
            pltpu.VMEM(block, f32),
            pltpu.VMEM((ports, slots), jnp.bfloat16),
            *scratch,
            pltpu.VMEM((cells, slots), jnp.bfloat16),
            pltpu.VMEM((cells, slots), f32),
            pltpu.VMEM((depth_z, slots), jnp.bfloat16),
            pltpu.VMEM((slots, depth_z), jnp.bfloat16),
            pltpu.VMEM((steps, slots), f32),
            pltpu.VMEM((steps, slots), f32),
            pltpu.VMEM(block, f32),
            pltpu.VMEM((steps, 1, ports), f32),
            pltpu.VMEM((count_y, chunk, 1, ports), f32),
            pltpu.VMEM((count_x, chunk, 1, ports), f32),
            pltpu.VMEM((steps, 1, ports), f32),
            pltpu.VMEM((TAIL, ports), f32),
            pltpu.VMEM((count_y, TAIL, ports), f32),
            pltpu.VMEM((count_x, TAIL, ports), f32),
            pltpu.SemaphoreType.DMA((7,)),
            pltpu.SemaphoreType.DMA((2,)),
            pltpu.SemaphoreType.DMA((len(KINDS),)),
            pltpu.SemaphoreType.DMA((len(KINDS), SLOTS)),
            pltpu.SemaphoreType.DMA((len(COEFFICIENTS),)),
            pltpu.SemaphoreType.DMA((len(COEFFICIENTS),)),
            pltpu.SemaphoreType.DMA((transfers,)),
            pltpu.SemaphoreType.DMA((transfers,)),
            pltpu.SemaphoreType.DMA((count_x + count_y,)),
            pltpu.SemaphoreType.DMA((count_x + count_y,)),
        ],
        compiler_params=pltpu.CompilerParams(
            collective_id=0, has_side_effects=True, vmem_limit_bytes=60 * 1024 * 1024
        ),
    )(
        electric, magnetic, aux_electric, aux_magnetic, grades, permittivity,
        dipole_cell, dipole_port.reshape(1, slots), live_count, injection, waveform.T,
    )
    return electric, magnetic, power


def solution(mesh):
    in_specs = (
        P(None, "gx", "gy", None),
        P(None, "gx", "gy", None),
        P(None, "gx", "gy", None),
        P(None, "gx", "gy", None),
        P(None, "gx", "gy", None),
        P("gx", "gy", None),
        P(None, ("gx", "gy")),
        P(("gx", "gy")),
        P(("gx", "gy")),
        P(("gx", "gy"), None),
        P(),
    )
    out_specs = (P(None, "gx", "gy", None), P(None, "gx", "gy", None), P())
    return jax.shard_map(local, mesh=mesh, in_specs=in_specs, out_specs=out_specs, check_vma=False)
```

```python
import functools

import jax
import jax.numpy as jnp
from jax import lax
from jax.experimental import pallas as pl
from jax.experimental.pallas import tpu as pltpu
from jax.sharding import PartitionSpec as P

MESH = pl.DeviceIdType.MESH
courant = 0.55
absorb_keep = (0.0, 0.92, 0.75, 0.45)
absorb_take = (0.0, -0.06, -0.18, -0.35)
derivative_pairs = ((2, 1), (1, 2), (0, 2), (2, 0), (1, 0), (0, 1))
UNROLL = 8
TAIL = 4


def grade_table(grades, table):
    result = jnp.where(grades == 1, table[1], 0.0)
    result = jnp.where(grades == 2, table[2], result)
    return jnp.where(grades == 3, table[3], result)


def split_two(values):
    high = values.astype(jnp.bfloat16)
    low = (values - high.astype(jnp.float32)).astype(jnp.bfloat16)
    return high, low


KINDS = ("ay", "by", "axh", "axl", "bxl", "bxh", "d1", "d2")
TRAVEL = {
    "ay": (0, 1), "by": (0, -1), "axh": (1, 0), "axl": (1, 0),
    "bxl": (-1, 0), "bxh": (-1, 0), "d1": (-1, 1), "d2": (1, -1),
}
COEFFICIENTS = ((0, 1), (0, -1), (1, 0), (-1, 0), (-1, 1), (1, -1))
SLOTS = 4


def kernel(
    e_in, h_in, me_in, mh_in, grades_ref, eps_ref, cell_ref, port_ref, live_ref, inj_ref, wave_ref,
    ef, hf, power_ref,
    me, mh, grades, eps, inj, keep, take, factor, source, member,
    say, sby, saxh, saxl, sbxl, sbxh, sd1, sd2,
    ray, rby, raxh, raxl, rbxl, rbxh, rd1, rd2,
    cs_up, cs_down, cs_right, cs_left, cs_d1, cs_d2,
    cr_up, cr_down, cr_right, cr_left, cr_d1, cr_d2,
    row_h, row_e, save_row_h, save_row_e, save_h_lo, save_h_hi, save_e_lo, save_e_hi, lines,
    edge_h, edge_ht, edge_e, edge_et,
    cell_t, cell_f, depth_t, depth, current, record, z_copy,
    share, from_y, from_x, result, late, late_y, late_x,
    load_sem, send_sem, recv_sem, send_one, recv_one, send_sum, recv_sum, send_late, recv_late,
):
    depth_x, depth_y, depth_z = eps_ref.shape
    ports, slots = inj_ref.shape[1], inj_ref.shape[0]
    steps = wave_ref.shape[0]
    half = depth_y // 2
    last_x, last_y = depth_x - 1, depth_y - 1
    ix, iy = lax.axis_index("gx"), lax.axis_index("gy")
    count_x, count_y = lax.axis_size("gx"), lax.axis_size("gy")
    f32 = jnp.float32

    def there(dx, dy):
        found = ix >= 0
        if dx:
            found = jnp.logical_and(found, ix > 0 if dx < 0 else ix < count_x - 1)
        if dy:
            found = jnp.logical_and(found, iy > 0 if dy < 0 else iy < count_y - 1)
        return found

    loads = [
        pltpu.make_async_copy(e_in, ef.at[:, pl.ds(0, depth_x)], load_sem.at[0]),
        pltpu.make_async_copy(grades_ref, grades, load_sem.at[1]),
        pltpu.make_async_copy(eps_ref, eps, load_sem.at[2]),
        pltpu.make_async_copy(h_in, hf.at[:, pl.ds(1, depth_x)], load_sem.at[3]),
        pltpu.make_async_copy(me_in, me, load_sem.at[4]),
        pltpu.make_async_copy(mh_in, mh, load_sem.at[5]),
        pltpu.make_async_copy(inj_ref, inj, load_sem.at[6]),
    ]
    for copy in loads:
        copy.start()
    record[...] = jnp.zeros(record.shape, f32)

    plane = jnp.zeros((depth_y, depth_z), f32)
    for component in range(3):
        ef[component, depth_x] = plane
        hf[component, 0] = plane
    for ref in (
        ray, rby, raxh, raxl, rbxl, rbxh, rd1, rd2,
        cr_up, cr_down, cr_right, cr_left, cr_d1, cr_d2,
        save_row_h, save_h_lo, save_h_hi, lines, sd2, cs_up, cs_down, cs_right, cs_left, cs_d1, cs_d2,
    ):
        ref[...] = jnp.zeros(ref.shape, f32)

    barrier = pltpu.get_barrier_semaphore()
    line_x = [(lax.rem(ix + offset, count_x), iy) for offset in range(1, count_x)]
    line_y = [(ix, lax.rem(iy + offset, count_y)) for offset in range(1, count_y)]
    across = [
        (lax.rem(ix + count_x - 1, count_x), lax.rem(iy + 1, count_y)),
        (lax.rem(ix + 1, count_x), lax.rem(iy + count_y - 1, count_y)),
    ]
    for peer in line_x + line_y + across:
        pl.semaphore_signal(barrier, inc=1, device_id=peer, device_id_type=MESH)

    once = []
    for number, (source_ref, target_ref) in enumerate((
        (cs_up, cr_up), (cs_down, cr_down), (cs_right, cr_right),
        (cs_left, cr_left), (cs_d1, cr_d1), (cs_d2, cr_d2),
    )):
        dx, dy = COEFFICIENTS[number]
        once.append((there(dx, dy), there(-dx, -dy), pltpu.make_async_remote_copy(
            src_ref=source_ref, dst_ref=target_ref,
            send_sem=send_one.at[number], recv_sem=recv_one.at[number],
            device_id=(ix + dx, iy + dy), device_id_type=MESH)))

    sends = dict(ay=say, by=sby, axh=saxh, axl=saxl, bxl=sbxl, bxh=sbxh, d1=sd1, d2=sd2)
    gets = dict(ay=ray, by=rby, axh=raxh, axl=raxl, bxl=rbxl, bxh=rbxh, d1=rd1, d2=rd2)

    def message(kind, step):
        number = KINDS.index(kind)
        slot = lax.rem(step, SLOTS)
        dx, dy = TRAVEL[kind]
        return pltpu.make_async_remote_copy(
            src_ref=sends[kind], dst_ref=gets[kind].at[slot],
            send_sem=send_sem.at[number], recv_sem=recv_sem.at[number, slot],
            device_id=(ix + dx, iy + dy), device_id_type=MESH)

    def send(step, *kinds):
        for kind in kinds:
            dx, dy = TRAVEL[kind]
            pl.when(there(dx, dy))(message(kind, step).start)

    def sent(step, *kinds):
        for kind in kinds:
            dx, dy = TRAVEL[kind]
            pl.when(there(dx, dy))(message(kind, step).wait_send)

    def arrived(step, *kinds):
        for kind in kinds:
            dx, dy = TRAVEL[kind]
            pl.when(there(-dx, -dy))(message(kind, step).wait_recv)

    low, high = slice(0, half), slice(half, depth_y)
    loads[0].wait()

    for x in range(depth_x):
        sby[0, x:x + 1, :] = ef[0, x, 0:1, :]
        sby[1, x:x + 1, :] = ef[2, x, 0:1, :]
    for c in (1, 2):
        sbxl[c - 1] = ef[c, 0, low]
        sbxh[c - 1] = ef[c, 0, high]
    sd2[1:2, :] = ef[0, last_x, 0:1, :]
    pl.semaphore_wait(barrier, len(line_x) + len(line_y) + len(across))
    send(0, "by", "bxl", "bxh", "d2")
    save_row_e[...] = sby[...]
    save_e_lo[...] = sbxl[...]
    save_e_hi[...] = sbxh[...]
    def prepare(x, _):
        for d in range(3):
            level = grades[d, x]
            keep[d, x] = grade_table(level, absorb_keep)
            take[d, x] = grade_table(level, absorb_take)
        factor[x] = courant / eps[x]
        return 0

    for copy in loads[1:3]:
        copy.wait()
    lax.fori_loop(0, depth_x, prepare, 0)

    row_half = lax.broadcasted_iota(jnp.int32, (half, depth_z), 0)
    is_top, is_bottom = row_half == half - 1, row_half == 0

    for x in range(depth_x):
        upper = take[1, x, half:, :]
        lower = take[1, x, :half, :]
        scale_h = courant * (1.0 + upper)
        scale_e = factor[x, :half, :] * (1.0 + lower)
        edge_h[x] = jnp.where(is_top, scale_h, 0.0)
        edge_ht[x] = jnp.where(is_top, upper, 0.0)
        edge_e[x] = jnp.where(is_bottom, scale_e, 0.0)
        edge_et[x] = jnp.where(is_bottom, lower, 0.0)
        cs_up[x:x + 1, :] = scale_h[half - 1:half, :]
        cs_down[x:x + 1, :] = scale_e[0:1, :]
    cs_right[0:depth_y, :] = courant * (1.0 + take[0, last_x])
    cs_left[0:depth_y, :] = factor[0] * (1.0 + take[0, 0])
    cs_up[depth_x:depth_x + 1, :] = cs_right[last_y:depth_y, :]
    cs_down[depth_x:depth_x + 1, :] = cs_left[0:1, :]
    cs_right[depth_y:depth_y + 1, :] = cs_up[last_x:depth_x, :]
    cs_left[depth_y:depth_y + 1, :] = cs_down[0:1, :]
    cs_d1[0:1, :] = cs_up[0:1, :]
    cs_d2[0:1, :] = cs_down[last_x:depth_x, :]

    for wanted, _, copy in once:
        pl.when(wanted)(copy.start)
    lanes = lax.broadcasted_iota(jnp.int32, (half, depth_z), 1)
    z_last, z_first = lanes == depth_z - 1, lanes == 0

    def curl(x, part, here, beside, line, memory, forward):
        turn_y = half - 1 if forward else 1
        turn_z = depth_z - 1 if forward else 1
        edge_y = is_top if forward else is_bottom
        edge_z = z_last if forward else z_first
        terms = []
        for number, (component, axis) in enumerate(derivative_pairs):
            value = here[component]
            if axis == 0:
                other = beside[component]
            elif axis == 1:
                other = jnp.where(edge_y, line[component], pltpu.roll(value, turn_y, 0))
            else:
                other = jnp.where(edge_z, 0.0, pltpu.roll(value, turn_z, 1))
            slope = other - value if forward else value - other
            carried = keep[axis, x, part] * memory[number, x, part] + take[axis, x, part] * slope
            memory[number, x, part] = carried
            terms.append(slope + carried)
        return (terms[0] - terms[1], terms[2] - terms[3], terms[4] - terms[5])

    blocks = depth_x // UNROLL
    no_line = [0.0, None, 0.0]

    def update_h(upper):
        part = high if upper else low

        def run(block, _):
            for inner in range(UNROLL):
                x = block * UNROLL + inner
                here = [ef[c, x, part] for c in range(3)]
                beside = [None, ef[1, x + 1, part], ef[2, x + 1, part]]
                line = no_line
                if not upper:
                    line = [ef[0, x, half:half + 1, :], None, ef[2, x, half:half + 1, :]]
                rotation = curl(x, part, here, beside, line, me, True)
                fresh = [hf[c, x + 1, part] - courant * rotation[c] for c in range(3)]
                for c in range(3):
                    hf[c, x + 1, part] = fresh[c]
                z_copy[x, part] = here[2]
                if upper:
                    say[0, pl.ds(x, 1), :] = fresh[0][half - 1:half, :]
                    say[1, pl.ds(x, 1), :] = fresh[2][half - 1:half, :]
            return 0

        lax.fori_loop(0, blocks, run, 0)

    def update_e(upper):
        part = high if upper else low

        def run(block, _):
            for inner in range(UNROLL):
                x = block * UNROLL + inner
                here = [hf[c, x + 1, part] for c in range(3)]
                beside = [None, hf[1, x, part], hf[2, x, part]]
                line = no_line
                if upper:
                    line = [hf[0, x + 1, half - 1:half, :], None, hf[2, x + 1, half - 1:half, :]]
                rotation = curl(x, part, here, beside, line, mh, False)
                ratio = factor[x, part]
                fresh = [ef[c, x, part] + ratio * rotation[c] for c in range(3)]
                fresh[2] = fresh[2] - source[x, part]
                for c in range(3):
                    ef[c, x, part] = fresh[c]
                if not upper:
                    sby[0, pl.ds(x, 1), :] = fresh[0][0:1, :]
                    sby[1, pl.ds(x, 1), :] = fresh[2][0:1, :]
            return 0

        lax.fori_loop(0, blocks, run, 0)

    def fix_h_side(part, side_y, side_z):
        scale = cs_right[part]
        amount = take[0, last_x, part]
        hf[1, depth_x, part] = hf[1, depth_x, part] + scale * side_z
        hf[2, depth_x, part] = hf[2, depth_x, part] - scale * side_y
        me[3, last_x, part] = me[3, last_x, part] + amount * side_z
        me[4, last_x, part] = me[4, last_x, part] + amount * side_y

    def fix_e_side(part, side_y, side_z):
        scale = cs_left[part]
        amount = take[0, 0, part]
        ef[1, 0, part] = ef[1, 0, part] + scale * side_z
        ef[2, 0, part] = ef[2, 0, part] - scale * side_y
        mh[3, 0, part] = mh[3, 0, part] - amount * side_z
        mh[4, 0, part] = mh[4, 0, part] - amount * side_y

    ey_corner, hx_corner, ez_edge, ex_corner, hz_edge = (pl.ds(8 * n, 1) for n in range(5))
    rows_x, rows_y = pl.ds(0, depth_x), pl.ds(0, depth_y)

    def settle_e_low(step):
        arrived(step, "ay", "d1", "axl")
        slot = lax.rem(step, SLOTS)
        scale = cr_up[rows_x]
        below_x = ray[slot, 0] - scale * save_row_e[1]
        below_z = ray[slot, 1] + scale * save_row_e[0]
        row_h[0] = below_x
        row_h[1] = below_z
        row_h[1, last_x:depth_x, :] = (
            row_h[1, last_x:depth_x, :] - cr_up[depth_x:depth_x + 1, :] * rd1[slot, 1:2, :])
        scale = cr_right[low]
        side_y = raxl[slot, 0] + scale * save_e_lo[1]
        side_z = raxl[slot, 1] - scale * save_e_lo[0]
        lines[hx_corner] = rd1[slot, 0:1, :] - cr_d1[0:1, :] * lines[ez_edge]
        fix_e_side(low, side_y, side_z)
        for x in range(depth_x):
            line_hx, line_hz = row_h[0, x:x + 1, :], row_h[1, x:x + 1, :]
            amount, scale = edge_et[x], edge_e[x]
            ef[0, x, low] = ef[0, x, low] - scale * line_hz
            ef[2, x, low] = ef[2, x, low] + scale * line_hx
            mh[0, x, low] = mh[0, x, low] - amount * line_hz
            mh[5, x, low] = mh[5, x, low] - amount * line_hx
        scale = cs_down[rows_x]
        save_row_e[0] = sby[0] - scale * row_h[1]
        save_row_e[1] = sby[1] + scale * row_h[0]
        save_row_e[1, 0:1, :] = save_row_e[1, 0:1, :] - cs_down[depth_x:depth_x + 1, :] * side_y[0:1, :]
        save_e_lo[0] = ef[1, 0, low]
        save_e_lo[1] = ef[2, 0, low]

    def settle_h_low(step, first):
        arrived(step, "bxl")
        slot = lax.rem(step, SLOTS)
        side_y, side_z = rbxl[slot, 0], rbxl[slot, 1]
        if not first:
            scale = cr_left[low]
            side_y = side_y + scale * save_h_lo[1]
            side_z = side_z - scale * save_h_lo[0]
            corner = cr_left[depth_y:depth_y + 1, :] * lines[hx_corner]
            side_z = side_z + jnp.where(is_bottom, corner, 0.0)
        lines[ez_edge] = side_z[0:1, :]
        fix_h_side(low, side_y, side_z)
        save_h_lo[0] = hf[1, depth_x, low]
        save_h_lo[1] = hf[2, depth_x, low]
        sd2[0:1, :] = hf[1, depth_x, 0:1, :]

    def settle_h_high(step, first):
        arrived(step, "by", "d2", "bxh")
        slot = lax.rem(step, SLOTS)
        side_y, side_z = rbxh[slot, 0], rbxh[slot, 1]
        if first:
            row_e[...] = rby[slot]
            lines[ex_corner] = rd2[slot, 1:2, :]
        else:
            scale = cr_down[rows_x]
            row_e[0] = rby[slot, 0] - scale * save_row_h[1]
            row_e[1] = rby[slot, 1] + scale * save_row_h[0]
            row_e[1, 0:1, :] = (
                row_e[1, 0:1, :] - cr_down[depth_x:depth_x + 1, :] * rd2[slot, 0:1, :])
            scale = cr_left[high]
            side_y = side_y + scale * save_h_hi[1]
            side_z = side_z - scale * save_h_hi[0]
            lines[ex_corner] = rd2[slot, 1:2, :] - cr_d2[0:1, :] * lines[hz_edge]
        fix_h_side(high, side_y, side_z)
        for x in range(depth_x):
            line_ex, line_ez = row_e[0, x:x + 1, :], row_e[1, x:x + 1, :]
            amount, scale = edge_ht[x], edge_h[x]
            hf[0, x + 1, high] = hf[0, x + 1, high] - scale * line_ez
            hf[2, x + 1, high] = hf[2, x + 1, high] + scale * line_ex
            me[0, x, high] = me[0, x, high] + amount * line_ez
            me[5, x, high] = me[5, x, high] + amount * line_ex
        scale = cs_up[rows_x]
        save_row_h[0] = say[0] - scale * row_e[1]
        save_row_h[1] = say[1] + scale * row_e[0]
        save_row_h[1, last_x:depth_x, :] = (
            save_row_h[1, last_x:depth_x, :] - cs_up[depth_x:depth_x + 1, :] * side_y[half - 1:half, :])
        save_h_hi[0] = hf[1, depth_x, high]
        save_h_hi[1] = hf[2, depth_x, high]

    def settle_e_high(step):
        arrived(step, "axh")
        slot = lax.rem(step, SLOTS)
        scale = cr_right[high]
        side_y = raxh[slot, 0] + scale * save_e_hi[1]
        side_z = raxh[slot, 1] - scale * save_e_hi[0]
        corner = cr_right[depth_y:depth_y + 1, :] * lines[ex_corner]
        side_z = side_z + jnp.where(is_top, corner, 0.0)
        lines[hz_edge] = side_z[half - 1:half, :]
        fix_e_side(high, side_y, side_z)
        save_e_hi[0] = ef[1, 0, high]
        save_e_hi[1] = ef[2, 0, high]

    def inject(step):
        top, rest = split_two(courant * current[pl.ds(step, 1), :])
        total = None
        for part in (top, rest):
            piece = jnp.dot(
                cell_t[...] * part, depth[...], preferred_element_type=jnp.float32
            )
            total = piece if total is None else total + piece
        source[...] = total.reshape(source.shape)

    def read_out(values, step):
        top, rest = split_two(values.reshape(depth_x * depth_y, depth_z))
        picked = jnp.dot(top, depth_t[...], preferred_element_type=jnp.float32)
        picked = picked + jnp.dot(rest, depth_t[...], preferred_element_type=jnp.float32)
        chosen = jnp.sum(picked * cell_f[...], axis=0, keepdims=True)
        record[pl.ds(step, 1), :] = chosen * current[pl.ds(step, 1), :]

    cells = (cell_ref[0:1, :] - ix * depth_x) * depth_y + (cell_ref[1:2, :] - iy * depth_y)
    hit = lax.broadcasted_iota(jnp.int32, cell_f.shape, 0) == cells
    cell_f[...] = jnp.where(hit, 1.0, 0.0)
    cell_t[...] = jnp.where(hit, 1.0, 0.0).astype(jnp.bfloat16)
    hit = lax.broadcasted_iota(jnp.int32, depth_t.shape, 0) == cell_ref[2:3, :]
    table = jnp.where(hit, 1.0, 0.0)
    depth_t[...] = table.astype(jnp.bfloat16)
    depth[...] = table.T.astype(jnp.bfloat16)
    live = lax.broadcasted_iota(jnp.int32, (1, slots), 1) < live_ref[0]
    loads[6].wait()
    flow = lax.dot_general(
        wave_ref[...], inj[...], (((1,), (1,)), ((), ())), preferred_element_type=jnp.float32
    )
    current[...] = jnp.where(live, flow, 0.0)
    hit = lax.broadcasted_iota(jnp.int32, (ports, slots), 0) == port_ref[...]
    member[...] = jnp.where(hit, 1.0, 0.0).astype(jnp.bfloat16)


    for copy in loads[3:6]:
        copy.wait()

    def port_sums():
        total = None
        for part in split_two(record[...]):
            piece = lax.dot_general(
                part, member[...], (((1,), (1,)), ((), ())), preferred_element_type=f32
            )
            total = piece if total is None else total + piece
        return total

    chunk = steps // count_y
    mine = pl.ds(iy * chunk, chunk)

    def spread(sems, first, peers, source_of, target):
        return [
            pltpu.make_async_remote_copy(
                src_ref=source_of(peer), dst_ref=target,
                send_sem=sems[0].at[first + number], recv_sem=sems[1].at[first + number],
                device_id=peer, device_id_type=MESH)
            for number, peer in enumerate(peers)
        ]

    def launch(moves):
        for move in moves:
            move.start()

    def settle(moves):
        for move in moves:
            move.wait()

    sums = (send_sum, recv_sum)

    def first_moves():
        return spread(
            sums, 0, line_y, lambda peer: share.at[pl.ds(peer[1] * chunk, chunk)], from_y.at[iy])

    def second_moves():
        return spread(sums, len(line_y), line_x, lambda peer: from_x.at[ix], from_x.at[ix])

    def third_moves():
        first = len(line_y) + len(line_x)
        return spread(sums, first, line_y, lambda peer: result.at[mine], result.at[mine])

    def reduce_one():
        total = port_sums()
        for row in range(steps):
            share[row] = total[row:row + 1, :]
        launch(first_moves())
        from_y[iy] = share[mine]

    def reduce_two():
        settle(first_moves())
        from_x[ix] = sum(from_y[j] for j in range(count_y))
        launch(second_moves())

    def reduce_three():
        settle(second_moves())
        result[mine] = sum(from_x[i] for i in range(count_x))
        launch(third_moves())

    def turn(step, _):
        more = step < steps
        update_h(True)
        for c in (1, 2):
            saxh[c - 1] = hf[c, depth_x, high]
        sd1[0:1, :] = say[0, 0:1, :]
        sd1[1:2, :] = ef[1, 0, last_y:depth_y, :]
        send(step, "d1", "ay", "axh")
        inject(step - 1)
        pl.when(step > 1)(lambda: settle_e_low(step - 1))
        update_h(False)
        for c in (1, 2):
            saxl[c - 1] = hf[c, depth_x, low]
        send(step, "axl")
        sent(step - 1, "by", "bxl", "d2")

        pl.when(step == 1)(lambda: settle_h_low(step - 1, True))
        pl.when(step > 1)(lambda: settle_h_low(step - 1, False))
        update_e(False)
        for c in (1, 2):
            sbxl[c - 1] = ef[c, 0, low]
        sd2[1:2, :] = sby[0, last_x:depth_x, :]
        pl.when(more)(lambda: send(step, "d2", "by", "bxl"))
        read_out(z_copy[...], lax.rem(step + steps - 2, steps))
        pl.when(step == steps - TAIL + 1)(reduce_one)
        pl.when(step == steps - TAIL + 3)(reduce_two)
        pl.when(step == steps - TAIL + 4)(reduce_three)
        sent(step - 1, "bxh")
        pl.when(step == 1)(lambda: settle_h_high(step - 1, True))
        pl.when(step > 1)(lambda: settle_h_high(step - 1, False))
        update_e(True)
        for c in (1, 2):
            sbxh[c - 1] = ef[c, 0, high]
        pl.when(more)(lambda: send(step, "bxh"))
        sent(step, "ay", "axh", "d1", "axl")

        @pl.when(step == 1)
        def _():
            for wanted, expected, copy in once:
                pl.when(wanted)(copy.wait_send)
                pl.when(expected)(copy.wait_recv)

        settle_e_high(step)
        return 0

    lax.fori_loop(1, steps + 1, turn, 0)
    settle_e_low(steps)
    read_out(ef[2, pl.ds(0, depth_x)], steps - 1)
    late[...] = port_sums()[steps - TAIL:, :]
    lates = (send_late, recv_late)
    moves = spread(lates, 0, line_y, lambda peer: late, late_y.at[iy])
    launch(moves)
    late_y[iy] = late[...]
    settle(third_moves())
    for row in range(steps - TAIL):
        power_ref[row:row + 1, :] = result[row]
    settle(moves)
    late_x[ix] = sum(late_y[j] for j in range(count_y))
    moves = spread(lates, len(line_y), line_x, lambda peer: late_x.at[ix], late_x.at[ix])
    launch(moves)
    settle(moves)
    power_ref[steps - TAIL:, :] = sum(late_x[i] for i in range(count_x))


def store_kernel(ef, hf, power_ref, e_out, h_out, power_out, sem):
    depth_x = e_out.shape[1]
    copies = [
        pltpu.make_async_copy(ef.at[:, pl.ds(0, depth_x)], e_out, sem.at[0]),
        pltpu.make_async_copy(hf.at[:, pl.ds(1, depth_x)], h_out, sem.at[1]),
        pltpu.make_async_copy(power_ref, power_out, sem.at[2]),
    ]
    for copy in copies:
        copy.start()
    for copy in copies:
        copy.wait()


def local(
    electric, magnetic, aux_electric, aux_magnetic, grades, permittivity,
    dipole_cell, dipole_port, live_count, injection, waveform,
):
    depth_x, depth_y, depth_z = permittivity.shape
    slots = dipole_cell.shape[1]
    ports, steps = waveform.shape
    block = (depth_x, depth_y, depth_z)
    cells = depth_x * depth_y
    f32 = jnp.float32
    count_x, count_y = lax.axis_size("gx"), lax.axis_size("gy")
    chunk = steps // count_y
    assert chunk * count_y == steps
    transfers = count_x + 2 * count_y
    half = depth_y // 2
    row = (2, depth_x, depth_z)
    side = (2, half, depth_z)
    pair = (2, depth_z)
    messages = (row, row, side, side, side, side, pair, pair)
    tall, wide, single = (depth_x + 8, depth_z), (depth_y + 8, depth_z), (8, depth_z)
    coefficients = (tall, tall, wide, wide, single, single)
    shapes = (
        messages + tuple((SLOTS,) + shape for shape in messages) + coefficients + coefficients
        + (row,) * 4 + (side,) * 4 + ((40, depth_z),) + ((depth_x, half, depth_z),) * 4
    )
    scratch = [pltpu.VMEM(shape, f32) for shape in shapes]
    vmem = pl.BlockSpec(memory_space=pltpu.VMEM)
    anywhere = pl.BlockSpec(memory_space=pltpu.HBM)
    fields = pl.pallas_call(
        kernel,
        out_shape=(
            pltpu.VMEM((3, depth_x + 1, depth_y, depth_z), f32),
            pltpu.VMEM((3, depth_x + 1, depth_y, depth_z), f32),
            pltpu.VMEM((steps, ports), f32),
        ),
        in_specs=[anywhere] * 6 + [vmem] * 2
        + [pl.BlockSpec(memory_space=pltpu.SMEM), anywhere, vmem],
        out_specs=(vmem, vmem, vmem),
        scratch_shapes=[
            pltpu.VMEM((6,) + block, f32),
            pltpu.VMEM((6,) + block, f32),
            pltpu.VMEM((3,) + block, jnp.int32),
            pltpu.VMEM(block, f32),
            pltpu.VMEM((slots, ports), jnp.bfloat16),
            pltpu.VMEM((3,) + block, f32),
            pltpu.VMEM((3,) + block, f32),
            pltpu.VMEM(block, f32),
            pltpu.VMEM(block, f32),
            pltpu.VMEM((ports, slots), jnp.bfloat16),
            *scratch,
            pltpu.VMEM((cells, slots), jnp.bfloat16),
            pltpu.VMEM((cells, slots), f32),
            pltpu.VMEM((depth_z, slots), jnp.bfloat16),
            pltpu.VMEM((slots, depth_z), jnp.bfloat16),
            pltpu.VMEM((steps, slots), f32),
            pltpu.VMEM((steps, slots), f32),
            pltpu.VMEM(block, f32),
            pltpu.VMEM((steps, 1, ports), f32),
            pltpu.VMEM((count_y, chunk, 1, ports), f32),
            pltpu.VMEM((count_x, chunk, 1, ports), f32),
            pltpu.VMEM((steps, 1, ports), f32),
            pltpu.VMEM((TAIL, ports), f32),
            pltpu.VMEM((count_y, TAIL, ports), f32),
            pltpu.VMEM((count_x, TAIL, ports), f32),
            pltpu.SemaphoreType.DMA((7,)),
            pltpu.SemaphoreType.DMA((len(KINDS),)),
            pltpu.SemaphoreType.DMA((len(KINDS), SLOTS)),
            pltpu.SemaphoreType.DMA((len(COEFFICIENTS),)),
            pltpu.SemaphoreType.DMA((len(COEFFICIENTS),)),
            pltpu.SemaphoreType.DMA((transfers,)),
            pltpu.SemaphoreType.DMA((transfers,)),
            pltpu.SemaphoreType.DMA((count_x + count_y,)),
            pltpu.SemaphoreType.DMA((count_x + count_y,)),
        ],
        compiler_params=pltpu.CompilerParams(
            collective_id=0, has_side_effects=True, vmem_limit_bytes=60 * 1024 * 1024
        ),
    )(
        electric, magnetic, aux_electric, aux_magnetic, grades, permittivity,
        dipole_cell, dipole_port.reshape(1, slots), live_count, injection, waveform.T,
    )
    return pl.pallas_call(
        store_kernel,
        out_shape=(
            jax.ShapeDtypeStruct(electric.shape, f32),
            jax.ShapeDtypeStruct(magnetic.shape, f32),
            jax.ShapeDtypeStruct((steps, ports), f32),
        ),
        in_specs=[vmem] * 3,
        out_specs=(anywhere,) * 3,
        scratch_shapes=[pltpu.SemaphoreType.DMA((3,))],
        compiler_params=pltpu.CompilerParams(vmem_limit_bytes=1024 * 1024),
    )(*fields)


def solution(mesh):
    in_specs = (
        P(None, "gx", "gy", None),
        P(None, "gx", "gy", None),
        P(None, "gx", "gy", None),
        P(None, "gx", "gy", None),
        P(None, "gx", "gy", None),
        P("gx", "gy", None),
        P(None, ("gx", "gy")),
        P(("gx", "gy")),
        P(("gx", "gy")),
        P(("gx", "gy"), None),
        P(),
    )
    out_specs = (P(None, "gx", "gy", None), P(None, "gx", "gy", None), P())
    return jax.shard_map(local, mesh=mesh, in_specs=in_specs, out_specs=out_specs, check_vma=False)
```

```python
import functools

import jax
import jax.numpy as jnp
from jax import lax
from jax.experimental import pallas as pl
from jax.experimental.pallas import tpu as pltpu
from jax.sharding import PartitionSpec as P

MESH = pl.DeviceIdType.MESH
courant = 0.55
absorb_keep = (0.0, 0.92, 0.75, 0.45)
absorb_take = (0.0, -0.06, -0.18, -0.35)
derivative_pairs = ((2, 1), (1, 2), (0, 2), (2, 0), (1, 0), (0, 1))
TAIL = 4


def grade_table(grades, table):
    result = jnp.where(grades == 1, table[1], 0.0)
    result = jnp.where(grades == 2, table[2], result)
    return jnp.where(grades == 3, table[3], result)


def split_two(values):
    high = values.astype(jnp.bfloat16)
    low = (values - high.astype(jnp.float32)).astype(jnp.bfloat16)
    return high, low


KINDS = ("ay", "by", "axh", "axl", "bxl", "bxh", "d1", "d2")
TRAVEL = {
    "ay": (0, 1), "by": (0, -1), "axh": (1, 0), "axl": (1, 0),
    "bxl": (-1, 0), "bxh": (-1, 0), "d1": (-1, 1), "d2": (1, -1),
}
COEFFICIENTS = ((0, 1), (0, -1), (1, 0), (-1, 0), (-1, 1), (1, -1))
SLOTS = 4


def kernel(
    e_in, h_in, me_in, mh_in, grades_ref, eps_ref, cell_ref, port_ref, live_ref, inj_ref, wave_ref,
    ef, hf, power_ref,
    me, mh, grades, eps, inj, keep, take, factor, source, member,
    say, sby, saxh, saxl, sbxl, sbxh, sd1, sd2,
    ray, rby, raxh, raxl, rbxl, rbxh, rd1, rd2,
    cs_up, cs_down, cs_right, cs_left, cs_d1, cs_d2,
    cr_up, cr_down, cr_right, cr_left, cr_d1, cr_d2,
    row_h, row_e, save_row_h, save_row_e, save_h_lo, save_h_hi, save_e_lo, save_e_hi, lines,
    edge_h, edge_ht, edge_e, edge_et,
    cell_t, cell_f, depth_t, depth, current, record, z_copy,
    share, from_y, from_x, result, late, late_y, late_x,
    load_sem, send_sem, recv_sem, send_one, recv_one, send_sum, recv_sum, send_late, recv_late,
):
    depth_x, depth_y, depth_z = eps_ref.shape
    ports, slots = inj_ref.shape[1], inj_ref.shape[0]
    steps = wave_ref.shape[0]
    half = depth_y // 2
    last_x, last_y = depth_x - 1, depth_y - 1
    ix, iy = lax.axis_index("gx"), lax.axis_index("gy")
    count_x, count_y = lax.axis_size("gx"), lax.axis_size("gy")
    f32 = jnp.float32

    def there(dx, dy):
        found = ix >= 0
        if dx:
            found = jnp.logical_and(found, ix > 0 if dx < 0 else ix < count_x - 1)
        if dy:
            found = jnp.logical_and(found, iy > 0 if dy < 0 else iy < count_y - 1)
        return found

    loads = [
        pltpu.make_async_copy(e_in, ef.at[:, pl.ds(0, depth_x)], load_sem.at[0]),
        pltpu.make_async_copy(grades_ref, grades, load_sem.at[1]),
        pltpu.make_async_copy(eps_ref, eps, load_sem.at[2]),
        pltpu.make_async_copy(h_in, hf.at[:, pl.ds(1, depth_x)], load_sem.at[3]),
        pltpu.make_async_copy(me_in, me, load_sem.at[4]),
        pltpu.make_async_copy(mh_in, mh, load_sem.at[5]),
        pltpu.make_async_copy(inj_ref, inj, load_sem.at[6]),
    ]
    for copy in loads:
        copy.start()
    record[...] = jnp.zeros(record.shape, f32)

    plane = jnp.zeros((depth_y, depth_z), f32)
    for component in range(3):
        ef[component, depth_x] = plane
        hf[component, 0] = plane
    for ref in (
        ray, rby, raxh, raxl, rbxl, rbxh, rd1, rd2,
        cr_up, cr_down, cr_right, cr_left, cr_d1, cr_d2,
        row_h, row_e, save_row_h, save_h_lo, save_h_hi, lines, sd2, cs_up, cs_down, cs_right, cs_left, cs_d1, cs_d2,
    ):
        ref[...] = jnp.zeros(ref.shape, f32)

    barrier = pltpu.get_barrier_semaphore()
    line_x = [(lax.rem(ix + offset, count_x), iy) for offset in range(1, count_x)]
    line_y = [(ix, lax.rem(iy + offset, count_y)) for offset in range(1, count_y)]
    across = [
        (lax.rem(ix + count_x - 1, count_x), lax.rem(iy + 1, count_y)),
        (lax.rem(ix + 1, count_x), lax.rem(iy + count_y - 1, count_y)),
    ]
    for peer in line_x + line_y + across:
        pl.semaphore_signal(barrier, inc=1, device_id=peer, device_id_type=MESH)

    once = []
    for number, (source_ref, target_ref) in enumerate((
        (cs_up, cr_up), (cs_down, cr_down), (cs_right, cr_right),
        (cs_left, cr_left), (cs_d1, cr_d1), (cs_d2, cr_d2),
    )):
        dx, dy = COEFFICIENTS[number]
        once.append((there(dx, dy), there(-dx, -dy), pltpu.make_async_remote_copy(
            src_ref=source_ref, dst_ref=target_ref,
            send_sem=send_one.at[number], recv_sem=recv_one.at[number],
            device_id=(ix + dx, iy + dy), device_id_type=MESH)))

    sends = dict(ay=say, by=sby, axh=saxh, axl=saxl, bxl=sbxl, bxh=sbxh, d1=sd1, d2=sd2)
    gets = dict(ay=ray, by=rby, axh=raxh, axl=raxl, bxl=rbxl, bxh=rbxh, d1=rd1, d2=rd2)

    def message(kind, step):
        number = KINDS.index(kind)
        slot = lax.rem(step, SLOTS)
        dx, dy = TRAVEL[kind]
        return pltpu.make_async_remote_copy(
            src_ref=sends[kind], dst_ref=gets[kind].at[slot],
            send_sem=send_sem.at[number], recv_sem=recv_sem.at[number, slot],
            device_id=(ix + dx, iy + dy), device_id_type=MESH)

    def send(step, *kinds):
        for kind in kinds:
            dx, dy = TRAVEL[kind]
            pl.when(there(dx, dy))(message(kind, step).start)

    def sent(step, *kinds):
        for kind in kinds:
            dx, dy = TRAVEL[kind]
            pl.when(there(dx, dy))(message(kind, step).wait_send)

    def arrived(step, *kinds):
        for kind in kinds:
            dx, dy = TRAVEL[kind]
            pl.when(there(-dx, -dy))(message(kind, step).wait_recv)

    low, high = slice(0, half), slice(half, depth_y)
    loads[0].wait()

    for x in range(depth_x):
        sby[0, x:x + 1, :] = ef[0, x, 0:1, :]
        sby[1, x:x + 1, :] = ef[2, x, 0:1, :]
    for c in (1, 2):
        sbxl[c - 1] = ef[c, 0, low]
        sbxh[c - 1] = ef[c, 0, high]
    sd2[1:2, :] = ef[0, last_x, 0:1, :]
    pl.semaphore_wait(barrier, len(line_x) + len(line_y) + len(across))
    send(0, "by", "bxl", "bxh", "d2")
    save_row_e[...] = sby[...]
    save_e_lo[...] = sbxl[...]
    save_e_hi[...] = sbxh[...]
    def prepare(x, _):
        for d in range(3):
            level = grades[d, x]
            keep[d, x] = grade_table(level, absorb_keep)
            take[d, x] = grade_table(level, absorb_take)
        factor[x] = courant / eps[x]
        return 0

    for copy in loads[1:3]:
        copy.wait()
    lax.fori_loop(0, depth_x, prepare, 0)

    row_half = lax.broadcasted_iota(jnp.int32, (half, depth_z), 0)
    is_top, is_bottom = row_half == half - 1, row_half == 0

    for x in range(depth_x):
        upper = take[1, x, half:, :]
        lower = take[1, x, :half, :]
        scale_h = courant * (1.0 + upper)
        scale_e = factor[x, :half, :] * (1.0 + lower)
        edge_h[x] = jnp.where(is_top, scale_h, 0.0)
        edge_ht[x] = jnp.where(is_top, upper, 0.0)
        edge_e[x] = jnp.where(is_bottom, scale_e, 0.0)
        edge_et[x] = jnp.where(is_bottom, lower, 0.0)
        cs_up[x:x + 1, :] = scale_h[half - 1:half, :]
        cs_down[x:x + 1, :] = scale_e[0:1, :]
    cs_right[0:depth_y, :] = courant * (1.0 + take[0, last_x])
    cs_left[0:depth_y, :] = factor[0] * (1.0 + take[0, 0])
    cs_up[depth_x:depth_x + 1, :] = cs_right[last_y:depth_y, :]
    cs_down[depth_x:depth_x + 1, :] = cs_left[0:1, :]
    cs_right[depth_y:depth_y + 1, :] = cs_up[last_x:depth_x, :]
    cs_left[depth_y:depth_y + 1, :] = cs_down[0:1, :]
    cs_d1[0:1, :] = cs_up[0:1, :]
    cs_d2[0:1, :] = cs_down[last_x:depth_x, :]

    for wanted, _, copy in once:
        pl.when(wanted)(copy.start)
    lanes = lax.broadcasted_iota(jnp.int32, (half, depth_z), 1)
    z_last, z_first = lanes == depth_z - 1, lanes == 0

    def curl(x, part, here, beside, line, memory, forward, extra):
        turn_y = half - 1 if forward else 1
        turn_z = depth_z - 1 if forward else 1
        edge_y = is_top if forward else is_bottom
        edge_z = z_last if forward else z_first
        terms = []
        for number, (component, axis) in enumerate(derivative_pairs):
            value = here[component]
            if axis == 0:
                other = beside[component]
            elif axis == 1:
                other = jnp.where(edge_y, line[component], pltpu.roll(value, turn_y, 0))
            else:
                other = jnp.where(edge_z, 0.0, pltpu.roll(value, turn_z, 1))
            slope = other - value if forward else value - other
            before = memory[number, x, part]
            if number in extra:
                before = before + extra[number]
            carried = keep[axis, x, part] * before + take[axis, x, part] * slope
            memory[number, x, part] = carried
            terms.append(slope + carried)
        return (terms[0] - terms[1], terms[2] - terms[3], terms[4] - terms[5])

    no_line = [0.0, None, 0.0]

    def update_h(upper):
        part = high if upper else low

        def fields(x):
            if upper or x == depth_x:
                return [ef[c, x, part] for c in range(3)]
            scale = edge_e[x]
            values = [
                ef[0, x, part] - scale * row_h[1, x:x + 1, :], ef[1, x, part],
                ef[2, x, part] + scale * row_h[0, x:x + 1, :]]
            ef[0, x, part] = values[0]
            ef[2, x, part] = values[2]
            return values

        here = fields(0)
        for x in range(depth_x):
            beside = fields(x + 1)
            line = no_line
            extra = {}
            if upper:
                amount = edge_ht[x]
                extra = {0: amount * row_e[1, x:x + 1, :], 5: amount * row_e[0, x:x + 1, :]}
            else:
                line = [ef[0, x, half:half + 1, :], None, ef[2, x, half:half + 1, :]]
            rotation = curl(x, part, here, beside, line, me, True, extra)
            fresh = [hf[c, x + 1, part] - courant * rotation[c] for c in range(3)]
            for c in range(3):
                hf[c, x + 1, part] = fresh[c]
            z_copy[x, part] = here[2]
            if upper:
                say[0, x:x + 1, :] = fresh[0][half - 1:half, :]
                say[1, x:x + 1, :] = fresh[2][half - 1:half, :]
            here = beside

    def update_e(upper):
        part = high if upper else low
        beside = [hf[c, 0, part] for c in range(3)]
        for x in range(depth_x):
            here = [hf[c, x + 1, part] for c in range(3)]
            line = no_line
            extra = {}
            if upper:
                scale = edge_h[x]
                here[0] = here[0] - scale * row_e[1, x:x + 1, :]
                here[2] = here[2] + scale * row_e[0, x:x + 1, :]
                hf[0, x + 1, part] = here[0]
                hf[2, x + 1, part] = here[2]
                line = [hf[0, x + 1, half - 1:half, :], None, hf[2, x + 1, half - 1:half, :]]
            else:
                amount = edge_et[x]
                extra = {0: -amount * row_h[1, x:x + 1, :], 5: -amount * row_h[0, x:x + 1, :]}
            rotation = curl(x, part, here, beside, line, mh, False, extra)
            ratio = factor[x, part]
            fresh = [ef[c, x, part] + ratio * rotation[c] for c in range(3)]
            fresh[2] = fresh[2] - source[x, part]
            for c in range(3):
                ef[c, x, part] = fresh[c]
            if not upper:
                sby[0, x:x + 1, :] = fresh[0][0:1, :]
                sby[1, x:x + 1, :] = fresh[2][0:1, :]
            beside = here

    def fix_h_side(part, side_y, side_z):
        scale = cs_right[part]
        amount = take[0, last_x, part]
        hf[1, depth_x, part] = hf[1, depth_x, part] + scale * side_z
        hf[2, depth_x, part] = hf[2, depth_x, part] - scale * side_y
        me[3, last_x, part] = me[3, last_x, part] + amount * side_z
        me[4, last_x, part] = me[4, last_x, part] + amount * side_y

    def fix_e_side(part, side_y, side_z):
        scale = cs_left[part]
        amount = take[0, 0, part]
        ef[1, 0, part] = ef[1, 0, part] + scale * side_z
        ef[2, 0, part] = ef[2, 0, part] - scale * side_y
        mh[3, 0, part] = mh[3, 0, part] - amount * side_z
        mh[4, 0, part] = mh[4, 0, part] - amount * side_y

    ey_corner, hx_corner, ez_edge, ex_corner, hz_edge = (pl.ds(8 * n, 1) for n in range(5))
    rows_x, rows_y = pl.ds(0, depth_x), pl.ds(0, depth_y)

    def settle_e_low(step):
        arrived(step, "ay", "d1", "axl")
        slot = lax.rem(step, SLOTS)
        scale = cr_up[rows_x]
        below_x = ray[slot, 0] - scale * save_row_e[1]
        below_z = ray[slot, 1] + scale * save_row_e[0]
        row_h[0] = below_x
        row_h[1] = below_z
        row_h[1, last_x:depth_x, :] = (
            row_h[1, last_x:depth_x, :] - cr_up[depth_x:depth_x + 1, :] * rd1[slot, 1:2, :])
        scale = cr_right[low]
        side_y = raxl[slot, 0] + scale * save_e_lo[1]
        side_z = raxl[slot, 1] - scale * save_e_lo[0]
        lines[hx_corner] = rd1[slot, 0:1, :] - cr_d1[0:1, :] * lines[ez_edge]
        fix_e_side(low, side_y, side_z)
        scale = cs_down[rows_x]
        save_row_e[0] = sby[0] - scale * row_h[1]
        save_row_e[1] = sby[1] + scale * row_h[0]
        save_row_e[1, 0:1, :] = save_row_e[1, 0:1, :] - cs_down[depth_x:depth_x + 1, :] * side_y[0:1, :]

    def settle_h_low(step, first):
        arrived(step, "bxl")
        slot = lax.rem(step, SLOTS)
        side_y, side_z = rbxl[slot, 0], rbxl[slot, 1]
        if not first:
            scale = cr_left[low]
            side_y = side_y + scale * save_h_lo[1]
            side_z = side_z - scale * save_h_lo[0]
            corner = cr_left[depth_y:depth_y + 1, :] * lines[hx_corner]
            side_z = side_z + jnp.where(is_bottom, corner, 0.0)
        lines[ez_edge] = side_z[0:1, :]
        fix_h_side(low, side_y, side_z)
        save_h_lo[0] = hf[1, depth_x, low]
        save_h_lo[1] = hf[2, depth_x, low]
        sd2[0:1, :] = hf[1, depth_x, 0:1, :]

    def settle_h_high(step, first):
        arrived(step, "by", "d2", "bxh")
        slot = lax.rem(step, SLOTS)
        side_y, side_z = rbxh[slot, 0], rbxh[slot, 1]
        if first:
            row_e[...] = rby[slot]
            lines[ex_corner] = rd2[slot, 1:2, :]
        else:
            scale = cr_down[rows_x]
            row_e[0] = rby[slot, 0] - scale * save_row_h[1]
            row_e[1] = rby[slot, 1] + scale * save_row_h[0]
            row_e[1, 0:1, :] = (
                row_e[1, 0:1, :] - cr_down[depth_x:depth_x + 1, :] * rd2[slot, 0:1, :])
            scale = cr_left[high]
            side_y = side_y + scale * save_h_hi[1]
            side_z = side_z - scale * save_h_hi[0]
            lines[ex_corner] = rd2[slot, 1:2, :] - cr_d2[0:1, :] * lines[hz_edge]
        fix_h_side(high, side_y, side_z)
        scale = cs_up[rows_x]
        save_row_h[0] = say[0] - scale * row_e[1]
        save_row_h[1] = say[1] + scale * row_e[0]
        save_row_h[1, last_x:depth_x, :] = (
            save_row_h[1, last_x:depth_x, :] - cs_up[depth_x:depth_x + 1, :] * side_y[half - 1:half, :])

    def settle_e_high(step):
        arrived(step, "axh")
        slot = lax.rem(step, SLOTS)
        scale = cr_right[high]
        side_y = raxh[slot, 0] + scale * save_e_hi[1]
        side_z = raxh[slot, 1] - scale * save_e_hi[0]
        corner = cr_right[depth_y:depth_y + 1, :] * lines[ex_corner]
        side_z = side_z + jnp.where(is_top, corner, 0.0)
        lines[hz_edge] = side_z[half - 1:half, :]
        fix_e_side(high, side_y, side_z)
        save_e_hi[0] = ef[1, 0, high]
        save_e_hi[1] = ef[2, 0, high]

    def inject(step):
        top, rest = split_two(courant * current[pl.ds(step, 1), :])
        both = jnp.concatenate([cell_t[...] * top, cell_t[...] * rest], axis=0)
        total = jnp.dot(both, depth[...], preferred_element_type=f32)
        total = total[:depth_x * depth_y] + total[depth_x * depth_y:]
        source[...] = total.reshape(source.shape)

    def read_out(values, step):
        count = depth_x * depth_y
        both = jnp.concatenate(split_two(values.reshape(count, depth_z)), axis=0)
        picked = jnp.dot(both, depth_t[...], preferred_element_type=f32)
        picked = picked[:count] + picked[count:]
        chosen = jnp.sum(picked * cell_f[...], axis=0, keepdims=True)
        record[pl.ds(step, 1), :] = chosen * current[pl.ds(step, 1), :]

    cells = (cell_ref[0:1, :] - ix * depth_x) * depth_y + (cell_ref[1:2, :] - iy * depth_y)
    hit = lax.broadcasted_iota(jnp.int32, cell_f.shape, 0) == cells
    cell_f[...] = jnp.where(hit, 1.0, 0.0)
    cell_t[...] = jnp.where(hit, 1.0, 0.0).astype(jnp.bfloat16)
    hit = lax.broadcasted_iota(jnp.int32, depth_t.shape, 0) == cell_ref[2:3, :]
    table = jnp.where(hit, 1.0, 0.0)
    depth_t[...] = table.astype(jnp.bfloat16)
    depth[...] = table.T.astype(jnp.bfloat16)
    live = lax.broadcasted_iota(jnp.int32, (1, slots), 1) < live_ref[0]
    loads[6].wait()
    flow = lax.dot_general(
        wave_ref[...], inj[...], (((1,), (1,)), ((), ())), preferred_element_type=jnp.float32
    )
    current[...] = jnp.where(live, flow, 0.0)
    hit = lax.broadcasted_iota(jnp.int32, (ports, slots), 0) == port_ref[...]
    member[...] = jnp.where(hit, 1.0, 0.0).astype(jnp.bfloat16)


    for copy in loads[3:6]:
        copy.wait()

    def port_sums():
        both = jnp.concatenate(split_two(record[...]), axis=0)
        total = lax.dot_general(
            both, member[...], (((1,), (1,)), ((), ())), preferred_element_type=f32
        )
        return total[:steps, :] + total[steps:, :]

    chunk = steps // count_y
    mine = pl.ds(iy * chunk, chunk)

    def spread(sems, first, peers, source_of, target):
        return [
            pltpu.make_async_remote_copy(
                src_ref=source_of(peer), dst_ref=target,
                send_sem=sems[0].at[first + number], recv_sem=sems[1].at[first + number],
                device_id=peer, device_id_type=MESH)
            for number, peer in enumerate(peers)
        ]

    def launch(moves):
        for move in moves:
            move.start()

    def settle(moves):
        for move in moves:
            move.wait()

    sums = (send_sum, recv_sum)

    def first_moves():
        return spread(
            sums, 0, line_y, lambda peer: share.at[pl.ds(peer[1] * chunk, chunk)], from_y.at[iy])

    def second_moves():
        return spread(sums, len(line_y), line_x, lambda peer: from_x.at[ix], from_x.at[ix])

    def third_moves():
        first = len(line_y) + len(line_x)
        return spread(sums, first, line_y, lambda peer: result.at[mine], result.at[mine])

    def reduce_one():
        total = port_sums()
        for row in range(steps):
            share[row] = total[row:row + 1, :]
        launch(first_moves())
        from_y[iy] = share[mine]

    def reduce_two():
        settle(first_moves())
        from_x[ix] = sum(from_y[j] for j in range(count_y))
        launch(second_moves())

    def reduce_three():
        settle(second_moves())
        result[mine] = sum(from_x[i] for i in range(count_x))
        launch(third_moves())

    def turn(step, _):
        more = step < steps
        update_h(True)
        for c in (1, 2):
            saxh[c - 1] = hf[c, depth_x, high]
        sd1[0:1, :] = say[0, 0:1, :]
        sd1[1:2, :] = ef[1, 0, last_y:depth_y, :]
        send(step, "d1", "ay", "axh")
        inject(step - 1)
        pl.when(step > 1)(lambda: settle_e_low(step - 1))
        update_h(False)
        save_e_lo[0] = ef[1, 0, low]
        save_e_lo[1] = ef[2, 0, low]
        for c in (1, 2):
            saxl[c - 1] = hf[c, depth_x, low]
        send(step, "axl")
        sent(step - 1, "by", "bxl", "d2")

        pl.when(step == 1)(lambda: settle_h_low(step - 1, True))
        pl.when(step > 1)(lambda: settle_h_low(step - 1, False))
        update_e(False)
        for c in (1, 2):
            sbxl[c - 1] = ef[c, 0, low]
        sd2[1:2, :] = sby[0, last_x:depth_x, :]
        pl.when(more)(lambda: send(step, "d2", "by", "bxl"))
        read_out(z_copy[...], lax.rem(step + steps - 2, steps))
        pl.when(step == steps - TAIL + 1)(reduce_one)
        pl.when(step == steps - TAIL + 3)(reduce_two)
        pl.when(step == steps - TAIL + 4)(reduce_three)
        sent(step - 1, "bxh")
        pl.when(step == 1)(lambda: settle_h_high(step - 1, True))
        pl.when(step > 1)(lambda: settle_h_high(step - 1, False))
        update_e(True)
        save_h_hi[0] = hf[1, depth_x, high]
        save_h_hi[1] = hf[2, depth_x, high]
        for c in (1, 2):
            sbxh[c - 1] = ef[c, 0, high]
        pl.when(more)(lambda: send(step, "bxh"))
        sent(step, "ay", "axh", "d1", "axl")

        @pl.when(step == 1)
        def _():
            for wanted, expected, copy in once:
                pl.when(wanted)(copy.wait_send)
                pl.when(expected)(copy.wait_recv)

        settle_e_high(step)
        return 0

    lax.fori_loop(1, steps + 1, turn, 0)
    settle_e_low(steps)
    for x in range(depth_x):
        scale = edge_e[x]
        ef[0, x, low] = ef[0, x, low] - scale * row_h[1, x:x + 1, :]
        ef[2, x, low] = ef[2, x, low] + scale * row_h[0, x:x + 1, :]
    read_out(ef[2, pl.ds(0, depth_x)], steps - 1)
    late[...] = port_sums()[steps - TAIL:, :]
    lates = (send_late, recv_late)
    moves = spread(lates, 0, line_y, lambda peer: late, late_y.at[iy])
    launch(moves)
    late_y[iy] = late[...]
    settle(third_moves())
    for row in range(steps - TAIL):
        power_ref[row:row + 1, :] = result[row]
    settle(moves)
    late_x[ix] = sum(late_y[j] for j in range(count_y))
    moves = spread(lates, len(line_y), line_x, lambda peer: late_x.at[ix], late_x.at[ix])
    launch(moves)
    settle(moves)
    power_ref[steps - TAIL:, :] = sum(late_x[i] for i in range(count_x))


def store_kernel(ef, hf, power_ref, e_out, h_out, power_out, sem):
    depth_x = e_out.shape[1]
    copies = [
        pltpu.make_async_copy(ef.at[:, pl.ds(0, depth_x)], e_out, sem.at[0]),
        pltpu.make_async_copy(hf.at[:, pl.ds(1, depth_x)], h_out, sem.at[1]),
        pltpu.make_async_copy(power_ref, power_out, sem.at[2]),
    ]
    for copy in copies:
        copy.start()
    for copy in copies:
        copy.wait()


def local(
    electric, magnetic, aux_electric, aux_magnetic, grades, permittivity,
    dipole_cell, dipole_port, live_count, injection, waveform,
):
    depth_x, depth_y, depth_z = permittivity.shape
    slots = dipole_cell.shape[1]
    ports, steps = waveform.shape
    block = (depth_x, depth_y, depth_z)
    cells = depth_x * depth_y
    f32 = jnp.float32
    count_x, count_y = lax.axis_size("gx"), lax.axis_size("gy")
    chunk = steps // count_y
    assert chunk * count_y == steps
    transfers = count_x + 2 * count_y
    half = depth_y // 2
    row = (2, depth_x, depth_z)
    side = (2, half, depth_z)
    pair = (2, depth_z)
    messages = (row, row, side, side, side, side, pair, pair)
    tall, wide, single = (depth_x + 8, depth_z), (depth_y + 8, depth_z), (8, depth_z)
    coefficients = (tall, tall, wide, wide, single, single)
    shapes = (
        messages + tuple((SLOTS,) + shape for shape in messages) + coefficients + coefficients
        + (row,) * 4 + (side,) * 4 + ((40, depth_z),) + ((depth_x, half, depth_z),) * 4
    )
    scratch = [pltpu.VMEM(shape, f32) for shape in shapes]
    vmem = pl.BlockSpec(memory_space=pltpu.VMEM)
    anywhere = pl.BlockSpec(memory_space=pltpu.HBM)
    fields = pl.pallas_call(
        kernel,
        out_shape=(
            pltpu.VMEM((3, depth_x + 1, depth_y, depth_z), f32),
            pltpu.VMEM((3, depth_x + 1, depth_y, depth_z), f32),
            pltpu.VMEM((steps, ports), f32),
        ),
        in_specs=[anywhere] * 6 + [vmem] * 2
        + [pl.BlockSpec(memory_space=pltpu.SMEM), anywhere, vmem],
        out_specs=(vmem, vmem, vmem),
        scratch_shapes=[
            pltpu.VMEM((6,) + block, f32),
            pltpu.VMEM((6,) + block, f32),
            pltpu.VMEM((3,) + block, jnp.int32),
            pltpu.VMEM(block, f32),
            pltpu.VMEM((slots, ports), jnp.bfloat16),
            pltpu.VMEM((3,) + block, f32),
            pltpu.VMEM((3,) + block, f32),
            pltpu.VMEM(block, f32),
            pltpu.VMEM(block, f32),
            pltpu.VMEM((ports, slots), jnp.bfloat16),
            *scratch,
            pltpu.VMEM((cells, slots), jnp.bfloat16),
            pltpu.VMEM((cells, slots), f32),
            pltpu.VMEM((depth_z, slots), jnp.bfloat16),
            pltpu.VMEM((slots, depth_z), jnp.bfloat16),
            pltpu.VMEM((steps, slots), f32),
            pltpu.VMEM((steps, slots), f32),
            pltpu.VMEM(block, f32),
            pltpu.VMEM((steps, 1, ports), f32),
            pltpu.VMEM((count_y, chunk, 1, ports), f32),
            pltpu.VMEM((count_x, chunk, 1, ports), f32),
            pltpu.VMEM((steps, 1, ports), f32),
            pltpu.VMEM((TAIL, ports), f32),
            pltpu.VMEM((count_y, TAIL, ports), f32),
            pltpu.VMEM((count_x, TAIL, ports), f32),
            pltpu.SemaphoreType.DMA((7,)),
            pltpu.SemaphoreType.DMA((len(KINDS),)),
            pltpu.SemaphoreType.DMA((len(KINDS), SLOTS)),
            pltpu.SemaphoreType.DMA((len(COEFFICIENTS),)),
            pltpu.SemaphoreType.DMA((len(COEFFICIENTS),)),
            pltpu.SemaphoreType.DMA((transfers,)),
            pltpu.SemaphoreType.DMA((transfers,)),
            pltpu.SemaphoreType.DMA((count_x + count_y,)),
            pltpu.SemaphoreType.DMA((count_x + count_y,)),
        ],
        compiler_params=pltpu.CompilerParams(
            collective_id=0, has_side_effects=True, vmem_limit_bytes=60 * 1024 * 1024
        ),
    )(
        electric, magnetic, aux_electric, aux_magnetic, grades, permittivity,
        dipole_cell, dipole_port.reshape(1, slots), live_count, injection, waveform.T,
    )
    return pl.pallas_call(
        store_kernel,
        out_shape=(
            jax.ShapeDtypeStruct(electric.shape, f32),
            jax.ShapeDtypeStruct(magnetic.shape, f32),
            jax.ShapeDtypeStruct((steps, ports), f32),
        ),
        in_specs=[vmem] * 3,
        out_specs=(anywhere,) * 3,
        scratch_shapes=[pltpu.SemaphoreType.DMA((3,))],
        compiler_params=pltpu.CompilerParams(vmem_limit_bytes=1024 * 1024),
    )(*fields)


def solution(mesh):
    in_specs = (
        P(None, "gx", "gy", None),
        P(None, "gx", "gy", None),
        P(None, "gx", "gy", None),
        P(None, "gx", "gy", None),
        P(None, "gx", "gy", None),
        P("gx", "gy", None),
        P(None, ("gx", "gy")),
        P(("gx", "gy")),
        P(("gx", "gy")),
        P(("gx", "gy"), None),
        P(),
    )
    out_specs = (P(None, "gx", "gy", None), P(None, "gx", "gy", None), P())
    return jax.shard_map(local, mesh=mesh, in_specs=in_specs, out_specs=out_specs, check_vma=False)
```

```python
import functools

import jax
import jax.numpy as jnp
from jax import lax
from jax.experimental import pallas as pl
from jax.experimental.pallas import tpu as pltpu
from jax.sharding import PartitionSpec as P

MESH = pl.DeviceIdType.MESH
courant = 0.55
absorb_keep = (0.0, 0.92, 0.75, 0.45)
absorb_take = (0.0, -0.06, -0.18, -0.35)
derivative_pairs = ((2, 1), (1, 2), (0, 2), (2, 0), (1, 0), (0, 1))
TAIL = 4


def grade_table(grades, table):
    result = jnp.where(grades == 1, table[1], 0.0)
    result = jnp.where(grades == 2, table[2], result)
    return jnp.where(grades == 3, table[3], result)


def split_two(values):
    high = values.astype(jnp.bfloat16)
    low = (values - high.astype(jnp.float32)).astype(jnp.bfloat16)
    return high, low


KINDS = ("ay", "by", "axh", "axl", "bxl", "bxh", "d1", "d2")
TRAVEL = {
    "ay": (0, 1), "by": (0, -1), "axh": (1, 0), "axl": (1, 0),
    "bxl": (-1, 0), "bxh": (-1, 0), "d1": (-1, 1), "d2": (1, -1),
}
COEFFICIENTS = ((0, 1), (0, -1), (1, 0), (-1, 0), (-1, 1), (1, -1))
SLOTS = 4


def kernel(
    e_in, h_in, me_in, mh_in, grades_ref, eps_ref, cell_ref, port_ref, live_ref, inj_ref, wave_ref,
    ef, hf, power_ref,
    me, mh, grades, eps, inj, keep, take, factor, source, member,
    say, sby, saxh, saxl, sbxl, sbxh, sd1, sd2,
    ray, rby, raxh, raxl, rbxl, rbxh, rd1, rd2,
    cs_up, cs_down, cs_right, cs_left, cs_d1, cs_d2,
    cr_up, cr_down, cr_right, cr_left, cr_d1, cr_d2,
    row_h, row_e, save_row_h, save_row_e, save_h_lo, save_h_hi, save_e_lo, save_e_hi, lines,
    edge_h, edge_ht, edge_e, edge_et,
    cell_t, cell_f, depth_t, depth, current, record, z_copy,
    share, from_y, from_x, result, late, late_y, late_x,
    load_sem, send_sem, recv_sem, send_one, recv_one, send_sum, recv_sum, send_late, recv_late,
):
    depth_x, depth_y, depth_z = eps_ref.shape
    ports, slots = inj_ref.shape[1], inj_ref.shape[0]
    steps = wave_ref.shape[0]
    half = depth_y // 2
    last_x, last_y = depth_x - 1, depth_y - 1
    ix, iy = lax.axis_index("gx"), lax.axis_index("gy")
    count_x, count_y = lax.axis_size("gx"), lax.axis_size("gy")
    f32 = jnp.float32

    def there(dx, dy):
        found = ix >= 0
        if dx:
            found = jnp.logical_and(found, ix > 0 if dx < 0 else ix < count_x - 1)
        if dy:
            found = jnp.logical_and(found, iy > 0 if dy < 0 else iy < count_y - 1)
        return found

    loads = [
        pltpu.make_async_copy(e_in, ef.at[:, pl.ds(0, depth_x)], load_sem.at[0]),
        pltpu.make_async_copy(grades_ref, grades, load_sem.at[1]),
        pltpu.make_async_copy(eps_ref, eps, load_sem.at[2]),
        pltpu.make_async_copy(h_in, hf.at[:, pl.ds(1, depth_x)], load_sem.at[3]),
        pltpu.make_async_copy(me_in, me, load_sem.at[4]),
        pltpu.make_async_copy(mh_in, mh, load_sem.at[5]),
        pltpu.make_async_copy(inj_ref, inj, load_sem.at[6]),
    ]
    for copy in loads:
        copy.start()
    record[...] = jnp.zeros(record.shape, f32)

    plane = jnp.zeros((depth_y, depth_z), f32)
    for component in range(3):
        ef[component, depth_x] = plane
        hf[component, 0] = plane
    for ref in (
        ray, rby, raxh, raxl, rbxl, rbxh, rd1, rd2,
        cr_up, cr_down, cr_right, cr_left, cr_d1, cr_d2,
        row_h, row_e, save_row_h, save_h_lo, save_h_hi, lines, sd2, cs_up, cs_down, cs_right, cs_left, cs_d1, cs_d2,
    ):
        ref[...] = jnp.zeros(ref.shape, f32)

    barrier = pltpu.get_barrier_semaphore()
    line_x = [(lax.rem(ix + offset, count_x), iy) for offset in range(1, count_x)]
    line_y = [(ix, lax.rem(iy + offset, count_y)) for offset in range(1, count_y)]
    across = [
        (lax.rem(ix + count_x - 1, count_x), lax.rem(iy + 1, count_y)),
        (lax.rem(ix + 1, count_x), lax.rem(iy + count_y - 1, count_y)),
    ]
    for peer in line_x + line_y + across:
        pl.semaphore_signal(barrier, inc=1, device_id=peer, device_id_type=MESH)

    once = []
    for number, (source_ref, target_ref) in enumerate((
        (cs_up, cr_up), (cs_down, cr_down), (cs_right, cr_right),
        (cs_left, cr_left), (cs_d1, cr_d1), (cs_d2, cr_d2),
    )):
        dx, dy = COEFFICIENTS[number]
        once.append((there(dx, dy), there(-dx, -dy), pltpu.make_async_remote_copy(
            src_ref=source_ref, dst_ref=target_ref,
            send_sem=send_one.at[number], recv_sem=recv_one.at[number],
            device_id=(ix + dx, iy + dy), device_id_type=MESH)))

    sends = dict(ay=say, by=sby, axh=saxh, axl=saxl, bxl=sbxl, bxh=sbxh, d1=sd1, d2=sd2)
    gets = dict(ay=ray, by=rby, axh=raxh, axl=raxl, bxl=rbxl, bxh=rbxh, d1=rd1, d2=rd2)

    def message(kind, step):
        number = KINDS.index(kind)
        slot = lax.rem(step, SLOTS)
        dx, dy = TRAVEL[kind]
        return pltpu.make_async_remote_copy(
            src_ref=sends[kind], dst_ref=gets[kind].at[slot],
            send_sem=send_sem.at[number], recv_sem=recv_sem.at[number, slot],
            device_id=(ix + dx, iy + dy), device_id_type=MESH)

    def send(step, *kinds):
        for kind in kinds:
            dx, dy = TRAVEL[kind]
            pl.when(there(dx, dy))(message(kind, step).start)

    def sent(step, *kinds):
        for kind in kinds:
            dx, dy = TRAVEL[kind]
            pl.when(there(dx, dy))(message(kind, step).wait_send)

    def arrived(step, *kinds):
        for kind in kinds:
            dx, dy = TRAVEL[kind]
            pl.when(there(-dx, -dy))(message(kind, step).wait_recv)

    low, high = slice(0, half), slice(half, depth_y)
    loads[0].wait()

    for x in range(depth_x):
        sby[0, x:x + 1, :] = ef[0, x, 0:1, :]
        sby[1, x:x + 1, :] = ef[2, x, 0:1, :]
    for c in (1, 2):
        sbxl[c - 1] = ef[c, 0, low]
        sbxh[c - 1] = ef[c, 0, high]
    sd2[1:2, :] = ef[0, last_x, 0:1, :]
    pl.semaphore_wait(barrier, len(line_x) + len(line_y) + len(across))
    send(0, "by", "bxl", "bxh", "d2")
    save_row_e[...] = sby[...]
    save_e_lo[...] = sbxl[...]
    save_e_hi[...] = sbxh[...]
    def prepare(x, _):
        for d in range(3):
            level = grades[d, x]
            keep[d, x] = grade_table(level, absorb_keep)
            take[d, x] = grade_table(level, absorb_take)
        factor[x] = courant / eps[x]
        return 0

    for copy in loads[1:3]:
        copy.wait()
    lax.fori_loop(0, depth_x, prepare, 0)

    row_half = lax.broadcasted_iota(jnp.int32, (half, depth_z), 0)
    is_top, is_bottom = row_half == half - 1, row_half == 0

    for x in range(depth_x):
        upper = take[1, x, half:, :]
        lower = take[1, x, :half, :]
        scale_h = courant * (1.0 + upper)
        scale_e = factor[x, :half, :] * (1.0 + lower)
        edge_h[x] = jnp.where(is_top, scale_h, 0.0)
        edge_ht[x] = jnp.where(is_top, upper, 0.0)
        edge_e[x] = jnp.where(is_bottom, scale_e, 0.0)
        edge_et[x] = jnp.where(is_bottom, lower, 0.0)
        cs_up[x:x + 1, :] = scale_h[half - 1:half, :]
        cs_down[x:x + 1, :] = scale_e[0:1, :]
    cs_right[0:depth_y, :] = courant * (1.0 + take[0, last_x])
    cs_left[0:depth_y, :] = factor[0] * (1.0 + take[0, 0])
    cs_up[depth_x:depth_x + 1, :] = cs_right[last_y:depth_y, :]
    cs_down[depth_x:depth_x + 1, :] = cs_left[0:1, :]
    cs_right[depth_y:depth_y + 1, :] = cs_up[last_x:depth_x, :]
    cs_left[depth_y:depth_y + 1, :] = cs_down[0:1, :]
    cs_d1[0:1, :] = cs_up[0:1, :]
    cs_d2[0:1, :] = cs_down[last_x:depth_x, :]

    for wanted, _, copy in once:
        pl.when(wanted)(copy.start)
    lanes = lax.broadcasted_iota(jnp.int32, (half, depth_z), 1)
    z_last, z_first = lanes == depth_z - 1, lanes == 0

    def curl(x, part, here, beside, line, memory, forward, extra):
        turn_y = half - 1 if forward else 1
        turn_z = depth_z - 1 if forward else 1
        edge_y = is_top if forward else is_bottom
        edge_z = z_last if forward else z_first
        terms = []
        for number, (component, axis) in enumerate(derivative_pairs):
            value = here[component]
            if axis == 0:
                other = beside[component]
            elif axis == 1:
                other = jnp.where(edge_y, line[component], pltpu.roll(value, turn_y, 0))
            else:
                other = jnp.where(edge_z, 0.0, pltpu.roll(value, turn_z, 1))
            slope = other - value if forward else value - other
            before = memory[number, x, part]
            if number in extra:
                before = before + extra[number]
            carried = keep[axis, x, part] * before + take[axis, x, part] * slope
            memory[number, x, part] = carried
            terms.append(slope + carried)
        return (terms[0] - terms[1], terms[2] - terms[3], terms[4] - terms[5])

    no_line = [0.0, None, 0.0]

    def update_h(upper):
        part = high if upper else low

        def fields(x):
            if upper or x == depth_x:
                return [ef[c, x, part] for c in range(3)]
            scale = edge_e[x]
            values = [
                ef[0, x, part] - scale * row_h[1, x:x + 1, :], ef[1, x, part],
                ef[2, x, part] + scale * row_h[0, x:x + 1, :]]
            ef[0, x, part] = values[0]
            ef[2, x, part] = values[2]
            return values

        here = fields(0)
        for x in range(depth_x):
            beside = fields(x + 1)
            line = no_line
            extra = {}
            if upper:
                amount = edge_ht[x]
                extra = {0: amount * row_e[1, x:x + 1, :], 5: amount * row_e[0, x:x + 1, :]}
            else:
                line = [ef[0, x, half:half + 1, :], None, ef[2, x, half:half + 1, :]]
            rotation = curl(x, part, here, beside, line, me, True, extra)
            fresh = [hf[c, x + 1, part] - courant * rotation[c] for c in range(3)]
            for c in range(3):
                hf[c, x + 1, part] = fresh[c]
            z_copy[x, part] = here[2]
            if upper:
                say[0, x:x + 1, :] = fresh[0][half - 1:half, :]
                say[1, x:x + 1, :] = fresh[2][half - 1:half, :]
            here = beside

    def update_e(upper):
        part = high if upper else low
        beside = [hf[c, 0, part] for c in range(3)]
        for x in range(depth_x):
            here = [hf[c, x + 1, part] for c in range(3)]
            line = no_line
            extra = {}
            if upper:
                scale = edge_h[x]
                here[0] = here[0] - scale * row_e[1, x:x + 1, :]
                here[2] = here[2] + scale * row_e[0, x:x + 1, :]
                hf[0, x + 1, part] = here[0]
                hf[2, x + 1, part] = here[2]
                line = [hf[0, x + 1, half - 1:half, :], None, hf[2, x + 1, half - 1:half, :]]
            else:
                amount = edge_et[x]
                extra = {0: -amount * row_h[1, x:x + 1, :], 5: -amount * row_h[0, x:x + 1, :]}
            rotation = curl(x, part, here, beside, line, mh, False, extra)
            ratio = factor[x, part]
            fresh = [ef[c, x, part] + ratio * rotation[c] for c in range(3)]
            fresh[2] = fresh[2] - source[x, part]
            for c in range(3):
                ef[c, x, part] = fresh[c]
            if not upper:
                sby[0, x:x + 1, :] = fresh[0][0:1, :]
                sby[1, x:x + 1, :] = fresh[2][0:1, :]
            beside = here

    def fix_h_side(part, side_y, side_z):
        scale = cs_right[part]
        amount = take[0, last_x, part]
        hf[1, depth_x, part] = hf[1, depth_x, part] + scale * side_z
        hf[2, depth_x, part] = hf[2, depth_x, part] - scale * side_y
        me[3, last_x, part] = me[3, last_x, part] + amount * side_z
        me[4, last_x, part] = me[4, last_x, part] + amount * side_y

    def fix_e_side(part, side_y, side_z):
        scale = cs_left[part]
        amount = take[0, 0, part]
        ef[1, 0, part] = ef[1, 0, part] + scale * side_z
        ef[2, 0, part] = ef[2, 0, part] - scale * side_y
        mh[3, 0, part] = mh[3, 0, part] - amount * side_z
        mh[4, 0, part] = mh[4, 0, part] - amount * side_y

    ey_corner, hx_corner, ez_edge, ex_corner, hz_edge = (pl.ds(8 * n, 1) for n in range(5))
    rows_x, rows_y = pl.ds(0, depth_x), pl.ds(0, depth_y)

    def settle_e_low(step):
        arrived(step, "ay", "d1", "axl")
        slot = lax.rem(step, SLOTS)
        scale = cr_up[rows_x]
        below_x = ray[slot, 0] - scale * save_row_e[1]
        below_z = ray[slot, 1] + scale * save_row_e[0]
        row_h[0] = below_x
        row_h[1] = below_z
        row_h[1, last_x:depth_x, :] = (
            row_h[1, last_x:depth_x, :] - cr_up[depth_x:depth_x + 1, :] * rd1[slot, 1:2, :])
        scale = cr_right[low]
        side_y = raxl[slot, 0] + scale * save_e_lo[1]
        side_z = raxl[slot, 1] - scale * save_e_lo[0]
        lines[hx_corner] = rd1[slot, 0:1, :] - cr_d1[0:1, :] * lines[ez_edge]
        fix_e_side(low, side_y, side_z)
        scale = cs_down[rows_x]
        save_row_e[0] = sby[0] - scale * row_h[1]
        save_row_e[1] = sby[1] + scale * row_h[0]
        save_row_e[1, 0:1, :] = save_row_e[1, 0:1, :] - cs_down[depth_x:depth_x + 1, :] * side_y[0:1, :]

    def settle_h_low(step, first):
        arrived(step, "bxl")
        slot = lax.rem(step, SLOTS)
        side_y, side_z = rbxl[slot, 0], rbxl[slot, 1]
        if not first:
            scale = cr_left[low]
            side_y = side_y + scale * save_h_lo[1]
            side_z = side_z - scale * save_h_lo[0]
            corner = cr_left[depth_y:depth_y + 1, :] * lines[hx_corner]
            side_z = side_z + jnp.where(is_bottom, corner, 0.0)
        lines[ez_edge] = side_z[0:1, :]
        fix_h_side(low, side_y, side_z)
        save_h_lo[0] = hf[1, depth_x, low]
        save_h_lo[1] = hf[2, depth_x, low]
        sd2[0:1, :] = hf[1, depth_x, 0:1, :]

    def settle_h_high(step, first):
        arrived(step, "by", "d2", "bxh")
        slot = lax.rem(step, SLOTS)
        side_y, side_z = rbxh[slot, 0], rbxh[slot, 1]
        if first:
            row_e[...] = rby[slot]
            lines[ex_corner] = rd2[slot, 1:2, :]
        else:
            scale = cr_down[rows_x]
            row_e[0] = rby[slot, 0] - scale * save_row_h[1]
            row_e[1] = rby[slot, 1] + scale * save_row_h[0]
            row_e[1, 0:1, :] = (
                row_e[1, 0:1, :] - cr_down[depth_x:depth_x + 1, :] * rd2[slot, 0:1, :])
            scale = cr_left[high]
            side_y = side_y + scale * save_h_hi[1]
            side_z = side_z - scale * save_h_hi[0]
            lines[ex_corner] = rd2[slot, 1:2, :] - cr_d2[0:1, :] * lines[hz_edge]
        fix_h_side(high, side_y, side_z)
        scale = cs_up[rows_x]
        save_row_h[0] = say[0] - scale * row_e[1]
        save_row_h[1] = say[1] + scale * row_e[0]
        save_row_h[1, last_x:depth_x, :] = (
            save_row_h[1, last_x:depth_x, :] - cs_up[depth_x:depth_x + 1, :] * side_y[half - 1:half, :])

    def settle_e_high(step):
        arrived(step, "axh")
        slot = lax.rem(step, SLOTS)
        scale = cr_right[high]
        side_y = raxh[slot, 0] + scale * save_e_hi[1]
        side_z = raxh[slot, 1] - scale * save_e_hi[0]
        corner = cr_right[depth_y:depth_y + 1, :] * lines[ex_corner]
        side_z = side_z + jnp.where(is_top, corner, 0.0)
        lines[hz_edge] = side_z[half - 1:half, :]
        fix_e_side(high, side_y, side_z)
        save_e_hi[0] = ef[1, 0, high]
        save_e_hi[1] = ef[2, 0, high]

    def inject(step):
        top, rest = split_two(courant * current[pl.ds(step, 1), :])
        both = jnp.concatenate([cell_t[...] * top, cell_t[...] * rest], axis=0)
        total = jnp.dot(both, depth[...], preferred_element_type=f32)
        total = total[:depth_x * depth_y] + total[depth_x * depth_y:]
        source[...] = total.reshape(source.shape)

    def read_out(values, step):
        count = depth_x * depth_y
        both = jnp.concatenate(split_two(values.reshape(count, depth_z)), axis=0)
        picked = jnp.dot(both, depth_t[...], preferred_element_type=f32)
        picked = picked[:count] + picked[count:]
        chosen = jnp.sum(picked * cell_f[...], axis=0, keepdims=True)
        record[pl.ds(step, 1), :] = chosen * current[pl.ds(step, 1), :]

    cells = (cell_ref[0:1, :] - ix * depth_x) * depth_y + (cell_ref[1:2, :] - iy * depth_y)
    hit = lax.broadcasted_iota(jnp.int32, cell_f.shape, 0) == cells
    cell_f[...] = jnp.where(hit, 1.0, 0.0)
    cell_t[...] = jnp.where(hit, 1.0, 0.0).astype(jnp.bfloat16)
    hit = lax.broadcasted_iota(jnp.int32, depth_t.shape, 0) == cell_ref[2:3, :]
    table = jnp.where(hit, 1.0, 0.0)
    depth_t[...] = table.astype(jnp.bfloat16)
    depth[...] = table.T.astype(jnp.bfloat16)
    live = lax.broadcasted_iota(jnp.int32, (1, slots), 1) < live_ref[0]
    loads[6].wait()
    flow = lax.dot_general(
        wave_ref[...], inj[...], (((1,), (1,)), ((), ())), preferred_element_type=jnp.float32
    )
    current[...] = jnp.where(live, flow, 0.0)
    hit = lax.broadcasted_iota(jnp.int32, (ports, slots), 0) == port_ref[...]
    member[...] = jnp.where(hit, 1.0, 0.0).astype(jnp.bfloat16)


    for copy in loads[3:6]:
        copy.wait()

    def port_sums():
        both = jnp.concatenate(split_two(record[...]), axis=0)
        total = lax.dot_general(
            both, member[...], (((1,), (1,)), ((), ())), preferred_element_type=f32
        )
        return total[:steps, :] + total[steps:, :]

    chunk = steps // count_y
    mine = pl.ds(iy * chunk, chunk)

    def spread(sems, first, peers, source_of, target):
        return [
            pltpu.make_async_remote_copy(
                src_ref=source_of(peer), dst_ref=target,
                send_sem=sems[0].at[first + number], recv_sem=sems[1].at[first + number],
                device_id=peer, device_id_type=MESH)
            for number, peer in enumerate(peers)
        ]

    def launch(moves):
        for move in moves:
            move.start()

    def settle(moves):
        for move in moves:
            move.wait()

    sums = (send_sum, recv_sum)

    def first_moves():
        return spread(
            sums, 0, line_y, lambda peer: share.at[pl.ds(peer[1] * chunk, chunk)], from_y.at[iy])

    def second_moves():
        return spread(sums, len(line_y), line_x, lambda peer: from_x.at[ix], from_x.at[ix])

    def third_moves():
        first = len(line_y) + len(line_x)
        return spread(sums, first, line_y, lambda peer: result.at[mine], result.at[mine])

    def reduce_one():
        total = port_sums()
        for row in range(steps):
            share[row] = total[row:row + 1, :]
        launch(first_moves())
        from_y[iy] = share[mine]

    def reduce_two():
        settle(first_moves())
        from_x[ix] = sum(from_y[j] for j in range(count_y))
        launch(second_moves())

    def reduce_three():
        settle(second_moves())
        result[mine] = sum(from_x[i] for i in range(count_x))
        launch(third_moves())

    def turn(step, _):
        more = step < steps
        update_h(True)
        for c in (1, 2):
            saxh[c - 1] = hf[c, depth_x, high]
        sd1[0:1, :] = say[0, 0:1, :]
        sd1[1:2, :] = ef[1, 0, last_y:depth_y, :]
        send(step, "d1", "axh", "ay")
        inject(step - 1)
        pl.when(step > 1)(lambda: settle_e_low(step - 1))
        update_h(False)
        save_e_lo[0] = ef[1, 0, low]
        save_e_lo[1] = ef[2, 0, low]
        for c in (1, 2):
            saxl[c - 1] = hf[c, depth_x, low]
        send(step, "axl")
        sent(step - 1, "by", "bxl", "d2")

        pl.when(step == 1)(lambda: settle_h_low(step - 1, True))
        pl.when(step > 1)(lambda: settle_h_low(step - 1, False))
        update_e(False)
        for c in (1, 2):
            sbxl[c - 1] = ef[c, 0, low]
        sd2[1:2, :] = sby[0, last_x:depth_x, :]
        pl.when(more)(lambda: send(step, "d2", "bxl", "by"))
        read_out(z_copy[...], lax.rem(step + steps - 2, steps))
        pl.when(step == steps - TAIL + 1)(reduce_one)
        pl.when(step == steps - TAIL + 3)(reduce_two)
        pl.when(step == steps - TAIL + 4)(reduce_three)
        sent(step - 1, "bxh")
        pl.when(step == 1)(lambda: settle_h_high(step - 1, True))
        pl.when(step > 1)(lambda: settle_h_high(step - 1, False))
        update_e(True)
        save_h_hi[0] = hf[1, depth_x, high]
        save_h_hi[1] = hf[2, depth_x, high]
        for c in (1, 2):
            sbxh[c - 1] = ef[c, 0, high]
        pl.when(more)(lambda: send(step, "bxh"))
        sent(step, "ay", "axh", "d1", "axl")

        @pl.when(step == 1)
        def _():
            for wanted, expected, copy in once:
                pl.when(wanted)(copy.wait_send)
                pl.when(expected)(copy.wait_recv)

        settle_e_high(step)
        return 0

    lax.fori_loop(1, steps + 1, turn, 0)
    settle_e_low(steps)
    for x in range(depth_x):
        scale = edge_e[x]
        ef[0, x, low] = ef[0, x, low] - scale * row_h[1, x:x + 1, :]
        ef[2, x, low] = ef[2, x, low] + scale * row_h[0, x:x + 1, :]
    read_out(ef[2, pl.ds(0, depth_x)], steps - 1)
    late[...] = port_sums()[steps - TAIL:, :]
    lates = (send_late, recv_late)
    moves = spread(lates, 0, line_y, lambda peer: late, late_y.at[iy])
    launch(moves)
    late_y[iy] = late[...]
    settle(third_moves())
    for row in range(steps - TAIL):
        power_ref[row:row + 1, :] = result[row]
    settle(moves)
    late_x[ix] = sum(late_y[j] for j in range(count_y))
    moves = spread(lates, len(line_y), line_x, lambda peer: late_x.at[ix], late_x.at[ix])
    launch(moves)
    settle(moves)
    power_ref[steps - TAIL:, :] = sum(late_x[i] for i in range(count_x))


def store_kernel(ef, hf, power_ref, e_out, h_out, power_out, sem):
    depth_x = e_out.shape[1]
    copies = [pltpu.make_async_copy(power_ref, power_out, sem.at[0])]
    for c in range(3):
        for number, (source_ref, first, target_ref) in enumerate(((ef, 0, e_out), (hf, 1, h_out))):
            copies.append(pltpu.make_async_copy(
                source_ref.at[c, pl.ds(first, depth_x)], target_ref.at[c],
                sem.at[1 + 2 * c + number]))
    for copy in copies:
        copy.start()
    for copy in copies:
        copy.wait()


def local(
    electric, magnetic, aux_electric, aux_magnetic, grades, permittivity,
    dipole_cell, dipole_port, live_count, injection, waveform,
):
    depth_x, depth_y, depth_z = permittivity.shape
    slots = dipole_cell.shape[1]
    ports, steps = waveform.shape
    block = (depth_x, depth_y, depth_z)
    cells = depth_x * depth_y
    f32 = jnp.float32
    count_x, count_y = lax.axis_size("gx"), lax.axis_size("gy")
    chunk = steps // count_y
    assert chunk * count_y == steps
    transfers = count_x + 2 * count_y
    half = depth_y // 2
    row = (2, depth_x, depth_z)
    side = (2, half, depth_z)
    pair = (2, depth_z)
    messages = (row, row, side, side, side, side, pair, pair)
    tall, wide, single = (depth_x + 8, depth_z), (depth_y + 8, depth_z), (8, depth_z)
    coefficients = (tall, tall, wide, wide, single, single)
    shapes = (
        messages + tuple((SLOTS,) + shape for shape in messages) + coefficients + coefficients
        + (row,) * 4 + (side,) * 4 + ((40, depth_z),) + ((depth_x, half, depth_z),) * 4
    )
    scratch = [pltpu.VMEM(shape, f32) for shape in shapes]
    vmem = pl.BlockSpec(memory_space=pltpu.VMEM)
    anywhere = pl.BlockSpec(memory_space=pltpu.HBM)
    fields = pl.pallas_call(
        kernel,
        out_shape=(
            pltpu.VMEM((3, depth_x + 1, depth_y, depth_z), f32),
            pltpu.VMEM((3, depth_x + 1, depth_y, depth_z), f32),
            pltpu.VMEM((steps, ports), f32),
        ),
        in_specs=[anywhere] * 6 + [vmem] * 2
        + [pl.BlockSpec(memory_space=pltpu.SMEM), anywhere, vmem],
        out_specs=(vmem, vmem, vmem),
        scratch_shapes=[
            pltpu.VMEM((6,) + block, f32),
            pltpu.VMEM((6,) + block, f32),
            pltpu.VMEM((3,) + block, jnp.int32),
            pltpu.VMEM(block, f32),
            pltpu.VMEM((slots, ports), jnp.bfloat16),
            pltpu.VMEM((3,) + block, f32),
            pltpu.VMEM((3,) + block, f32),
            pltpu.VMEM(block, f32),
            pltpu.VMEM(block, f32),
            pltpu.VMEM((ports, slots), jnp.bfloat16),
            *scratch,
            pltpu.VMEM((cells, slots), jnp.bfloat16),
            pltpu.VMEM((cells, slots), f32),
            pltpu.VMEM((depth_z, slots), jnp.bfloat16),
            pltpu.VMEM((slots, depth_z), jnp.bfloat16),
            pltpu.VMEM((steps, slots), f32),
            pltpu.VMEM((steps, slots), f32),
            pltpu.VMEM(block, f32),
            pltpu.VMEM((steps, 1, ports), f32),
            pltpu.VMEM((count_y, chunk, 1, ports), f32),
            pltpu.VMEM((count_x, chunk, 1, ports), f32),
            pltpu.VMEM((steps, 1, ports), f32),
            pltpu.VMEM((TAIL, ports), f32),
            pltpu.VMEM((count_y, TAIL, ports), f32),
            pltpu.VMEM((count_x, TAIL, ports), f32),
            pltpu.SemaphoreType.DMA((7,)),
            pltpu.SemaphoreType.DMA((len(KINDS),)),
            pltpu.SemaphoreType.DMA((len(KINDS), SLOTS)),
            pltpu.SemaphoreType.DMA((len(COEFFICIENTS),)),
            pltpu.SemaphoreType.DMA((len(COEFFICIENTS),)),
            pltpu.SemaphoreType.DMA((transfers,)),
            pltpu.SemaphoreType.DMA((transfers,)),
            pltpu.SemaphoreType.DMA((count_x + count_y,)),
            pltpu.SemaphoreType.DMA((count_x + count_y,)),
        ],
        compiler_params=pltpu.CompilerParams(
            collective_id=0, has_side_effects=True, vmem_limit_bytes=60 * 1024 * 1024
        ),
    )(
        electric, magnetic, aux_electric, aux_magnetic, grades, permittivity,
        dipole_cell, dipole_port.reshape(1, slots), live_count, injection, waveform.T,
    )
    return pl.pallas_call(
        store_kernel,
        out_shape=(
            jax.ShapeDtypeStruct(electric.shape, f32),
            jax.ShapeDtypeStruct(magnetic.shape, f32),
            jax.ShapeDtypeStruct((steps, ports), f32),
        ),
        in_specs=[vmem] * 3,
        out_specs=(anywhere,) * 3,
        scratch_shapes=[pltpu.SemaphoreType.DMA((7,))],
        compiler_params=pltpu.CompilerParams(vmem_limit_bytes=1024 * 1024),
    )(*fields)


def solution(mesh):
    in_specs = (
        P(None, "gx", "gy", None),
        P(None, "gx", "gy", None),
        P(None, "gx", "gy", None),
        P(None, "gx", "gy", None),
        P(None, "gx", "gy", None),
        P("gx", "gy", None),
        P(None, ("gx", "gy")),
        P(("gx", "gy")),
        P(("gx", "gy")),
        P(("gx", "gy"), None),
        P(),
    )
    out_specs = (P(None, "gx", "gy", None), P(None, "gx", "gy", None), P())
    return jax.shard_map(local, mesh=mesh, in_specs=in_specs, out_specs=out_specs, check_vma=False)
```
